64 devices in a mesh: data: 4 (over x, y), model: 16 (over z, core).
Axes of the slice: x: 2, y: 2, z: 8, core: 2. Of those that a mesh axis runs over, the one named last changes fastest.
The devices are a block of a 4x4x8 slice.
Arguments:
- queries: bfloat16 [256, 1536], P('data'), parts along dimension 0
- w_head: bfloat16 [1536, 151936], P(None, 'model')
- ds_keys: bfloat16 [262144, 1536], P('model')
- ds_tokens: int32 [262144], P('model')
- temperature: float32 [1], replicated
- mix_weight: float32 [1], replicated
Outputs:
- output: float32 [256, 151936], P('data', 'model'), parts along dimension 0
There are 4 independent parts. The reference program is written for one: setup_inputs(seed, part) draws one part's arguments, and reference() takes and returns one part's arrays. A program takes and returns all parts, laid end to end along the dimension named above; an argument that names none is the same for every part.
All inputs are finite; a program needn't handle non-finite values.
Results may differ from the reference program's by a relative error of at most 0.001.
Values are sent between devices in bfloat16 or wider.
A program may use at most 768 MiB of HBM per device.

```python
import jax
import jax.numpy as jnp
from jax import lax

Q_ROWS = 64
D_MODEL = 1536
VOCAB_SIZE = 151936
N_LOCAL = 16384
GROUP_SIZE = 16


def setup_inputs(seed: int = 0, part: int = 0) -> dict:
    root_key = jax.random.key(seed)
    key_query, key_head, key_store, key_token, key_temp, key_mix = jax.random.split(root_key, 6)
    key_query = jax.random.fold_in(key_query, part)
    n_total = GROUP_SIZE * N_LOCAL
    queries = jax.random.normal(key_query, (Q_ROWS, D_MODEL), jnp.float32)
    w_head = jax.random.normal(key_head, (D_MODEL, VOCAB_SIZE), jnp.float32) * (2.0 * D_MODEL ** -0.5)
    ds_keys = jax.random.normal(key_store, (n_total, D_MODEL), jnp.float32)
    ds_tokens = jax.random.randint(key_token, (n_total,), 0, VOCAB_SIZE, jnp.int32)
    ds_tokens = ds_tokens.at[0].set(VOCAB_SIZE - 1).at[1].set(0)
    temperature = jax.random.uniform(key_temp, (1,), jnp.float32, 0.7, 0.95) * (D_MODEL ** 0.5)
    mix_weight = jax.random.uniform(key_mix, (1,), jnp.float32, 0.25, 0.5)
    return {
        "queries": queries.astype(jnp.bfloat16),
        "w_head": w_head.astype(jnp.bfloat16),
        "ds_keys": ds_keys.astype(jnp.bfloat16),
        "ds_tokens": ds_tokens,
        "temperature": temperature,
        "mix_weight": mix_weight,
    }


def reference(queries, w_head, ds_keys, ds_tokens, temperature, mix_weight):
    key_blocks = ds_keys.reshape(GROUP_SIZE, N_LOCAL, D_MODEL)
    tok_blocks = ds_tokens.reshape(GROUP_SIZE, N_LOCAL)
    temp_value = temperature[0]

    def block_scores(key_block):
        cross_dot = jnp.dot(queries, key_block.T, preferred_element_type=jnp.float32)
        key_sq = jnp.sum(jnp.square(key_block.astype(jnp.float32)), axis=1)
        return (2.0 * cross_dot - key_sq[None, :]) / temp_value

    block_max = lax.map(lambda key_block: jnp.max(block_scores(key_block), axis=1), key_blocks)
    row_max = jnp.max(block_max, axis=0)

    def accumulate(carry_state, block_pair):
        histogram, row_total = carry_state
        key_block, tok_block = block_pair
        weights = jnp.exp(block_scores(key_block) - row_max[:, None])
        histogram = histogram.at[:, tok_block].add(weights)
        return (histogram, row_total + jnp.sum(weights, axis=1)), None

    start_state = (jnp.zeros((Q_ROWS, VOCAB_SIZE), jnp.float32), jnp.zeros((Q_ROWS,), jnp.float32))
    (histogram, row_total), unused = lax.scan(accumulate, start_state, (key_blocks, tok_blocks))
    logits = jnp.dot(queries, w_head, preferred_element_type=jnp.float32)
    lm_exp = jnp.exp(logits - jnp.max(logits, axis=1, keepdims=True))
    p_lm = lm_exp / jnp.sum(lm_exp, axis=1, keepdims=True)
    mix_value = mix_weight[0]
    return jnp.log(mix_value * histogram / row_total[:, None] + (1.0 - mix_value) * p_lm)
```

```python
import functools
import math

import jax
import jax.numpy as jnp
from jax import lax
from jax.experimental import pallas as pl
from jax.experimental.pallas import tpu as pltpu
from jax.sharding import PartitionSpec as P

MESH = pl.DeviceIdType.MESH
LANES = 128
KEY_TILE = 512
KEY_BUFS = 4
HEAD_TILE = 512
HEAD_BUFS = 3
VMEM_LIMIT = 60 * 1024 * 1024


def round_up(value, step):
    return (value + step - 1) // step * step


def slot_kernel(group, vocab, rows, starts_ref, tok_ref, ord_ref, col_ref, idx_ref):
    lane = lax.broadcasted_iota(jnp.int32, (rows, LANES), 1)
    slot = lax.broadcasted_iota(jnp.int32, (rows, LANES), 0) * LANES + lane
    for d in range(group):
        start = starts_ref[d]
        count = starts_ref[d + 1] - start
        row, off = start // LANES, lax.rem(start, LANES)
        shift = lax.rem(LANES - off, LANES)

        def shifted(ref):
            low = pltpu.roll(ref[pl.ds(row, rows), :], shift, 1)
            high = pltpu.roll(ref[pl.ds(row + 1, rows), :], shift, 1)
            return jnp.where(lane < LANES - off, low, high)

        used = slot < count
        col_ref[d] = jnp.where(used, shifted(tok_ref) - d * vocab, vocab)
        idx_ref[d] = jnp.where(used, shifted(ord_ref), 0)


def exchange_kernel(
    group, half, idx_ref, temp_ref, over_ref, query_ref, col_ref, key_hbm, head_hbm,
    recv_hbm, rcol_hbm, rstat_hbm, logit_ref,
    key_buf, head_buf, score, send, stat, key_sem, head_sem,
    data_send, data_recv, col_send, col_recv, stat_send, stat_recv, own_sem,
):
    me = lax.axis_index("model")
    n_local, vocab = key_hbm.shape[0], head_hbm.shape[0]
    slots = idx_ref.shape[0] // group

    barrier = pltpu.get_barrier_semaphore()
    for k in range(1, group):
        pl.semaphore_signal(
            barrier, inc=1, device_id={"model": lax.rem(me + k, group)}, device_id_type=MESH
        )

    def key_copy(step):
        return pltpu.make_async_copy(
            key_hbm.at[pl.ds(step * KEY_TILE, KEY_TILE), :],
            key_buf.at[lax.rem(step, KEY_BUFS)],
            key_sem.at[lax.rem(step, KEY_BUFS)],
        )

    head_full = vocab // HEAD_TILE
    head_rest = vocab - head_full * HEAD_TILE

    def head_copy(step):
        return pltpu.make_async_copy(
            head_hbm.at[pl.ds(step * HEAD_TILE, HEAD_TILE), :],
            head_buf.at[lax.rem(step, HEAD_BUFS)],
            head_sem.at[lax.rem(step, HEAD_BUFS)],
        )

    key_steps = n_local // KEY_TILE
    for step in range(KEY_BUFS - 1):
        key_copy(step).start()

    temp = temp_ref[0]

    def merge(total, tile):
        top, acc = total
        new = jnp.maximum(top, jnp.max(tile, axis=0, keepdims=True))
        acc = acc * jnp.exp(top - new) + jnp.sum(jnp.exp(tile - new), axis=0, keepdims=True)
        return new, acc

    empty = (jnp.full((1, LANES), -3e38, jnp.float32), jnp.zeros((1, LANES), jnp.float32))

    def score_step(step, total):
        @pl.when(step + KEY_BUFS - 1 < key_steps)
        def _():
            key_copy(step + KEY_BUFS - 1).start()

        key_copy(step).wait()
        keys = key_buf[lax.rem(step, KEY_BUFS)]
        cross = jnp.dot(keys, query_ref[...], preferred_element_type=jnp.float32)
        wide = keys.astype(jnp.float32)
        square = jnp.sum(wide * wide, axis=1, keepdims=True)
        tile = (2.0 * cross - square) / temp
        score[pl.ds(pl.multiple_of(step * KEY_TILE, KEY_TILE), KEY_TILE), :] = tile
        return merge(total, tile)

    knn_max, knn_sum = lax.fori_loop(0, key_steps, score_step, empty)

    for step in range(HEAD_BUFS - 1):
        head_copy(step).start()

    pl.semaphore_wait(barrier, group - 1)

    left = lax.broadcasted_iota(jnp.int32, (1, LANES), 1) < LANES // 2

    def pack(k, slot):
        base = lax.rem(me + k, group) * slots

        def rows(t, carry):
            for i in range(8):
                j = t * 8 + i
                a = idx_ref[base + j]
                b = idx_ref[base + half + j]
                row = jnp.where(left, score[pl.ds(a, 1), :], score[pl.ds(b, 1), :])
                send[slot, pl.ds(j, 1), :] = row
            return carry

        lax.fori_loop(0, half // 8, rows, 0)

    def data_copy(k):
        return pltpu.make_async_remote_copy(
            src_ref=send.at[k], dst_ref=recv_hbm.at[me],
            send_sem=data_send.at[k], recv_sem=data_recv.at[k],
            device_id={"model": lax.rem(me + k, group)}, device_id_type=MESH,
        )

    def cols_copy(k):
        return pltpu.make_async_remote_copy(
            src_ref=col_ref.at[lax.rem(me + k, group)], dst_ref=rcol_hbm.at[me],
            send_sem=col_send.at[k], recv_sem=col_recv.at[k],
            device_id={"model": lax.rem(me + k, group)}, device_id_type=MESH,
        )

    def stat_copy(k):
        return pltpu.make_async_remote_copy(
            src_ref=stat, dst_ref=rstat_hbm.at[me],
            send_sem=stat_send.at[k], recv_sem=stat_recv.at[k],
            device_id={"model": lax.rem(me + k, group)}, device_id_type=MESH,
        )

    mid = group // 2
    order = []
    for k in range(1, mid):
        order += [mid - k, mid + k] if k % 2 else [mid + k, mid - k]
    order = [mid] + order
    waiting = None
    for k in order:
        pack(k, k)
        if waiting is not None:
            data_copy(waiting).start()
        waiting = k
    pack(0, 0)
    data_copy(waiting).start()
    for k in order:
        cols_copy(k).start()

    def head_tile(rows_ref, where):
        tile = jnp.dot(rows_ref, query_ref[...], preferred_element_type=jnp.float32)
        logit_ref[where, :] = tile
        return tile

    rest_copy = pltpu.make_async_copy(
        head_hbm.at[pl.ds(head_full * HEAD_TILE, head_rest), :],
        head_buf.at[HEAD_BUFS, pl.ds(0, head_rest), :],
        head_sem.at[HEAD_BUFS],
    )
    if head_rest:
        rest_copy.start()

    def head_step(step, total):
        @pl.when(step + HEAD_BUFS - 1 < head_full)
        def _():
            head_copy(step + HEAD_BUFS - 1).start()

        head_copy(step).wait()
        where = pl.ds(pl.multiple_of(step * HEAD_TILE, HEAD_TILE), HEAD_TILE)
        return merge(total, head_tile(head_buf[lax.rem(step, HEAD_BUFS)], where))

    total = lax.fori_loop(0, head_full, head_step, empty)
    if head_rest:
        rest_copy.wait()
        where = pl.ds(head_full * HEAD_TILE, head_rest)
        total = merge(total, head_tile(head_buf[HEAD_BUFS, :head_rest, :], where))
    lm_max, lm_sum = total

    stat[0:1, :] = knn_max
    stat[1:2, :] = knn_sum
    stat[2:3, :] = lm_max
    stat[3:4, :] = lm_sum
    stat[4:8, :] = jnp.full((4, LANES), over_ref[0], jnp.float32)

    own = [
        pltpu.make_async_copy(send.at[0], recv_hbm.at[me], own_sem.at[0]),
        pltpu.make_async_copy(col_ref.at[me], rcol_hbm.at[me], own_sem.at[1]),
        pltpu.make_async_copy(stat, rstat_hbm.at[me], own_sem.at[2]),
    ]
    for copy in own:
        copy.start()
    for k in order:
        stat_copy(k).start()
    for copy in own:
        copy.wait()
    for k in order:
        stat_copy(k).wait()
        cols_copy(k).wait()
        data_copy(k).wait()


def finish_kernel(
    group, half, slots, col_ref, mix_ref, recv_ref, stat_ref, logit_ref, out_ref, sum_ref,
    weight, hist_a, hist_b, hist_c, hist_d,
):
    vocab = logit_ref.shape[0]
    hists = (hist_a, hist_b, hist_c, hist_d)

    def clear(i, carry):
        where = pl.ds(pl.multiple_of(i * 8, 8), 8)
        for hist in hists:
            hist[where, :] = jnp.zeros((8, LANES), jnp.float32)
        return carry

    lax.fori_loop(0, hist_a.shape[0] // 8, clear, 0)

    def combine(top_row):
        top = stat_ref[0, top_row : top_row + 1, :]
        for d in range(1, group):
            top = jnp.maximum(top, stat_ref[d, top_row : top_row + 1, :])
        acc = jnp.zeros((1, LANES), jnp.float32)
        for d in range(group):
            acc = acc + stat_ref[d, top_row + 1 : top_row + 2, :] * jnp.exp(
                stat_ref[d, top_row : top_row + 1, :] - top
            )
        return top, acc

    knn_max, knn_sum = combine(0)
    lm_max, lm_sum = combine(2)
    over = stat_ref[0, 4:5, :]
    for d in range(1, group):
        over = jnp.maximum(over, stat_ref[d, 4:5, :])
    sum_ref[0:1, :] = knn_max
    sum_ref[1:2, :] = knn_sum
    sum_ref[2:3, :] = lm_max
    sum_ref[3:4, :] = lm_sum
    sum_ref[4:8, :] = jnp.broadcast_to(over, (4, LANES))

    for d in range(group):

        def to_weight(i, carry):
            src = pl.ds(pl.multiple_of(i * 8, 8), 8)
            dst = pl.ds(pl.multiple_of(d * half + i * 8, 8), 8)
            weight[dst, :] = jnp.exp(recv_ref[d, src, :] - knn_max)
            return carry

        lax.fori_loop(0, half // 8, to_weight, 0)

    def add_rows(t, carry):
        d = t // (half // 8)
        j = (t - d * (half // 8)) * 8
        base = d * slots + j
        for i in range(8):
            row = weight[pl.ds(t * 8 + i, 1), :]
            low, high = hists[2 * (i % 2)], hists[2 * (i % 2) + 1]
            a = col_ref[base + i]
            low[pl.ds(a, 1), :] = low[pl.ds(a, 1), :] + row
            b = col_ref[base + half + i]
            high[pl.ds(b, 1), :] = high[pl.ds(b, 1), :] + row
        return carry

    lax.fori_loop(0, group * (half // 8), add_rows, 0)

    mix = mix_ref[0]
    knn_scale = mix / knn_sum
    lm_scale = (1.0 - mix) / lm_sum

    def tile(start, rows):
        where = pl.ds(start, rows)
        high = hist_b[where, :] + hist_d[where, :]
        hist = hist_a[where, :] + hist_c[where, :] + pltpu.roll(high, LANES // 2, 1)
        prob = hist * knn_scale + jnp.exp(logit_ref[where, :] - lm_max) * lm_scale
        return jnp.log(prob)

    full = vocab // LANES

    def write(i, carry):
        start = pl.multiple_of(i * LANES, LANES)
        out_ref[:, pl.ds(start, LANES)] = tile(start, LANES).T[: LANES // 2, :]
        return carry

    lax.fori_loop(0, full, write, 0)
    rest = vocab - full * LANES
    if rest:
        last = jnp.concatenate(
            [tile(full * LANES, rest), jnp.zeros((LANES - rest, LANES), jnp.float32)], axis=0
        )
        out_ref[:, full * LANES :] = last.T[: LANES // 2, :rest]


def solution(mesh):
    group = mesh.shape["model"]

    def local_step(queries, w_shard, key_shard, tok_shard, temperature, mix_weight):
        row_count, depth = queries.shape
        vocab, n_local = w_shard.shape[1], key_shard.shape[0]
        mean = n_local / group
        cap = round_up(int(mean + 4.5 * math.sqrt(mean)), 16)
        half = cap // 2
        slot_rows = round_up(cap, LANES) // LANES
        slots = slot_rows * LANES

        order_tok, order_idx = lax.sort(
            (tok_shard, lax.iota(jnp.int32, n_local)), num_keys=1, is_stable=False
        )
        bounds = jnp.arange(group + 1, dtype=jnp.int32) * vocab
        starts = jnp.sum(
            (tok_shard[None, :] < bounds[:, None]).astype(jnp.int32), axis=1
        )
        over = (jnp.max(starts[1:] - starts[:-1]) > cap).astype(jnp.float32).reshape(1)
        pad = (slot_rows + 8) * LANES
        fill = jnp.zeros((pad,), jnp.int32)
        shape_2d = ((n_local + pad) // LANES, LANES)
        tok_2d = jnp.concatenate([order_tok, fill]).reshape(shape_2d)
        idx_2d = jnp.concatenate([order_idx, fill]).reshape(shape_2d)

        smem = pl.BlockSpec(memory_space=pltpu.SMEM)
        vmem = pl.BlockSpec(memory_space=pltpu.VMEM)
        hbm = pl.BlockSpec(memory_space=pl.ANY)
        table = jax.ShapeDtypeStruct((group, slot_rows, LANES), jnp.int32)
        cols, idx = pl.pallas_call(
            functools.partial(slot_kernel, group, vocab, slot_rows),
            out_shape=(table, table),
            in_specs=[smem, vmem, vmem],
            out_specs=(vmem, vmem),
            name="slots",
        )(starts, tok_2d, idx_2d)

        query_t = jnp.concatenate([queries, queries], axis=0).T
        recv, rcols, rstat, logits = pl.pallas_call(
            functools.partial(exchange_kernel, group, half),
            out_shape=(
                jax.ShapeDtypeStruct((group, half, LANES), jnp.float32),
                table,
                jax.ShapeDtypeStruct((group, 8, LANES), jnp.float32),
                jax.ShapeDtypeStruct((vocab, LANES), jnp.float32),
            ),
            in_specs=[smem, smem, smem, vmem, vmem, hbm, hbm],
            out_specs=(hbm, hbm, hbm, vmem),
            scratch_shapes=[
                pltpu.VMEM((KEY_BUFS, KEY_TILE, depth), jnp.bfloat16),
                pltpu.VMEM((HEAD_BUFS + 1, HEAD_TILE, depth), jnp.bfloat16),
                pltpu.VMEM((n_local, LANES), jnp.float32),
                pltpu.VMEM((group, half, LANES), jnp.float32),
                pltpu.VMEM((8, LANES), jnp.float32),
                pltpu.SemaphoreType.DMA((KEY_BUFS,)),
                pltpu.SemaphoreType.DMA((HEAD_BUFS + 1,)),
                pltpu.SemaphoreType.DMA((group,)),
                pltpu.SemaphoreType.DMA((group,)),
                pltpu.SemaphoreType.DMA((group,)),
                pltpu.SemaphoreType.DMA((group,)),
                pltpu.SemaphoreType.DMA((group,)),
                pltpu.SemaphoreType.DMA((group,)),
                pltpu.SemaphoreType.DMA((3,)),
            ],
            compiler_params=pltpu.CompilerParams(
                collective_id=0, has_side_effects=True, vmem_limit_bytes=VMEM_LIMIT
            ),
            name="exchange",
        )(idx.reshape(-1), temperature, over, query_t, cols, key_shard, w_shard.T)

        hist_shape = pltpu.VMEM((round_up(vocab + 1, 8), LANES), jnp.float32)
        fast, sums = pl.pallas_call(
            functools.partial(finish_kernel, group, half, slots),
            out_shape=(
                jax.ShapeDtypeStruct((row_count, vocab), jnp.float32),
                jax.ShapeDtypeStruct((8, LANES), jnp.float32),
            ),
            in_specs=[smem, smem, vmem, vmem, vmem],
            out_specs=(vmem, vmem),
            scratch_shapes=[pltpu.VMEM((group * half, LANES), jnp.float32)] + [hist_shape] * 4,
            compiler_params=pltpu.CompilerParams(vmem_limit_bytes=VMEM_LIMIT),
            name="finish",
        )(rcols.reshape(-1), mix_weight, recv, rstat, logits)

        def dense(unused):
            me = lax.axis_index("model")
            row_max, row_total = sums[0, :row_count], sums[1, :row_count]
            lm_max, lm_total = sums[2, :row_count], sums[3, :row_count]
            cross_dot = jnp.einsum("bd,nd->nb", queries, key_shard, preferred_element_type=jnp.float32)
            key_sq = jnp.sum(jnp.square(key_shard.astype(jnp.float32)), axis=1)
            scores = (2.0 * cross_dot - key_sq[:, None]) / temperature[0]
            weights = jnp.exp(scores - row_max[None, :])
            ring = [(i, (i + 1) % group) for i in range(group)]

            def turn(k, acc):
                acc = lax.ppermute(acc, "model", ring)
                col = tok_shard - lax.rem(me + group - 1 - k, group) * vocab
                col = jnp.where((col >= 0) & (col < vocab), col, vocab)
                return acc.at[col].add(weights)

            acc = jnp.zeros((vocab + 1, row_count), jnp.float32)
            acc = lax.fori_loop(0, group, turn, acc)
            logit = jnp.dot(queries, w_shard, preferred_element_type=jnp.float32)
            p_lm = jnp.exp(logit - lm_max[:, None]) / lm_total[:, None]
            p_knn = acc[:vocab].T / row_total[:, None]
            mix_value = mix_weight[0]
            return jnp.log(mix_value * p_knn + (1.0 - mix_value) * p_lm)

        return lax.cond(sums[4, 0] > 0.0, dense, lambda kept: kept, fast)

    return jax.shard_map(
        local_step,
        mesh=mesh,
        in_specs=(P("data", None), P(None, "model"), P("model", None), P("model"), P(), P()),
        out_specs=P("data", "model"),
        check_vma=False,
    )
```

```python
import functools
import math

import jax
import jax.numpy as jnp
from jax import lax
from jax.experimental import pallas as pl
from jax.experimental.pallas import tpu as pltpu
from jax.sharding import PartitionSpec as P

MESH = pl.DeviceIdType.MESH
LANES = 128
KEY_TILE = 512
KEY_BUFS = 4
HEAD_TILE = 512
HEAD_BUFS = 3
COLS = 256
WINDOW = 64
BATCH = 4
VMEM_LIMIT = 60 * 1024 * 1024


def round_up(value, step):
    return (value + step - 1) // step * step


def slot_kernel(group, vocab, cap, rows, n_local, tok_ref, ord_ref, col_ref, idx_ref, off_ref, over_ref):
    lane = lax.broadcasted_iota(jnp.int32, (rows, LANES), 1)
    slot = lax.broadcasted_iota(jnp.int32, (rows, LANES), 0) * LANES + lane
    bound = lax.broadcasted_iota(jnp.int32, (LANES, LANES), 0)
    across = lax.broadcasted_iota(jnp.int32, (LANES, LANES), 1)
    tokens = tok_ref[: n_local // LANES, :]

    def below(limit):
        return jnp.sum((tokens < limit).astype(jnp.int32))

    starts = [0] + [below(d * vocab) for d in range(1, group)] + [n_local]
    table = jnp.zeros((LANES, LANES), jnp.float32)
    most = jnp.int32(0)
    for d in range(group):
        start, count = starts[d], starts[d + 1] - starts[d]
        most = jnp.maximum(most, count)
        row, off = start // LANES, start % LANES
        shift = (LANES - off) % LANES

        def shifted(ref):
            low = pltpu.roll(ref[pl.ds(row, rows), :], shift, 1)
            high = pltpu.roll(ref[pl.ds(row + 1, rows), :], shift, 1)
            return jnp.where(lane < LANES - off, low, high)

        used = slot < count
        col = jnp.where(used, shifted(tok_ref) - d * vocab, vocab)
        col_ref[d] = col
        idx_ref[d * rows : (d + 1) * rows, :] = jnp.where(used, shifted(ord_ref), 0)
        first = jnp.where(used, col // COLS, LANES)
        hits = jnp.zeros((LANES, LANES), jnp.float32)
        for r in range(rows):
            hits = hits + jnp.where(first[r : r + 1, :] < bound, 1.0, 0.0)
        table = jnp.where(across == d, jnp.sum(hits, axis=1, keepdims=True), table)
    widest = jnp.max(table[1:, :] - table[:-1, :])
    over = jnp.where((most > cap) | (widest > WINDOW), 1.0, 0.0)
    over_ref[...] = jnp.full((8, LANES), over, jnp.float32)
    turned = jnp.minimum(table, float(cap)).T.astype(jnp.int32)
    for d in range(group):
        off_ref[d] = turned[d : d + 1, :]


def exchange_kernel(
    group, half, rows, idx_ref, temp_ref, mix_ref, query_ref, over_ref, col_ref, off_ref, key_hbm, head_hbm,
    out_ref, sum_ref,
    key_buf, head_buf, turned, score, send, relay, recv, rcol, roff, off_smem, knn_stat, lm_stat, rknn, rlm,
    logit, hist, piece_a, piece_b,
    key_sem, head_sem, data_send, data_recv, relay_send, relay_recv, col_send, col_recv, off_send, off_recv,
    knn_send, knn_recv, lm_send, lm_recv, own_sem,
):
    me = lax.axis_index("model")
    n_local, vocab = key_hbm.shape[0], head_hbm.shape[0]
    slots = rows * LANES
    mid, quarter = group // 2, group // 4

    def peer(k):
        return {"model": lax.rem(me + k, group)}

    barrier = pltpu.get_barrier_semaphore()
    for k in range(1, group):
        pl.semaphore_signal(barrier, inc=1, device_id=peer(k), device_id_type=MESH)

    def key_copy(step):
        return pltpu.make_async_copy(
            key_hbm.at[pl.ds(step * KEY_TILE, KEY_TILE), :],
            key_buf.at[lax.rem(step, KEY_BUFS)],
            key_sem.at[lax.rem(step, KEY_BUFS)],
        )

    head_full = vocab // HEAD_TILE
    head_rest = vocab - head_full * HEAD_TILE

    def head_copy(step):
        return pltpu.make_async_copy(
            head_hbm.at[pl.ds(step * HEAD_TILE, HEAD_TILE), :],
            head_buf.at[lax.rem(step, HEAD_BUFS)],
            head_sem.at[lax.rem(step, HEAD_BUFS)],
        )

    key_steps = n_local // KEY_TILE
    for step in range(KEY_BUFS - 1):
        key_copy(step).start()

    temp = temp_ref[0]
    query = query_ref[...].astype(jnp.float32)
    turned[...] = jnp.concatenate([query, query], axis=0).T.astype(jnp.bfloat16)

    def merge(total, tile):
        top, acc = total
        new = jnp.maximum(top, jnp.max(tile, axis=0, keepdims=True))
        acc = acc * jnp.exp(top - new) + jnp.sum(jnp.exp(tile - new), axis=0, keepdims=True)
        return new, acc

    empty = (jnp.full((1, LANES), -3e38, jnp.float32), jnp.zeros((1, LANES), jnp.float32))

    def score_step(step, total):
        @pl.when(step + KEY_BUFS - 1 < key_steps)
        def _():
            key_copy(step + KEY_BUFS - 1).start()

        key_copy(step).wait()
        keys = key_buf[lax.rem(step, KEY_BUFS)]
        cross = jnp.dot(keys, turned[...], preferred_element_type=jnp.float32)
        wide = keys.astype(jnp.float32)
        square = jnp.sum(wide * wide, axis=1, keepdims=True)
        tile = (2.0 * cross - square) / temp
        score[pl.ds(pl.multiple_of(step * KEY_TILE, KEY_TILE), KEY_TILE), :] = tile
        return merge(total, tile)

    knn_max, knn_sum = lax.fori_loop(0, key_steps, score_step, empty)
    knn_stat[0:1, :] = knn_max
    knn_stat[1:2, :] = knn_sum
    knn_stat[2:8, :] = over_ref[2:8, :]

    for step in range(HEAD_BUFS - 1):
        head_copy(step).start()

    pl.semaphore_wait(barrier, group - 1)

    left = lax.broadcasted_iota(jnp.int32, (1, LANES), 1) < LANES // 2

    def remote(src, dst, send_sem, recv_sem, k):
        return pltpu.make_async_remote_copy(
            src_ref=src, dst_ref=dst, send_sem=send_sem, recv_sem=recv_sem,
            device_id=peer(k), device_id_type=MESH,
        )

    def data_copy(k):
        return remote(send.at[k], recv[k], data_send.at[k], data_recv.at[k], k)

    def cols_copy(k):
        return remote(col_ref.at[lax.rem(me + k, group)], rcol.at[k], col_send.at[k], col_recv.at[k], k)

    def offs_copy(k):
        return remote(off_ref.at[lax.rem(me + k, group)], roff.at[k], off_send.at[k], off_recv.at[k], k)

    def knn_copy(k):
        return remote(knn_stat, rknn.at[k], knn_send.at[k], knn_recv.at[k], k)

    def lm_copy(k):
        return remote(lm_stat, rlm.at[k], lm_send.at[k], lm_recv.at[k], k)

    first_leg = remote(send.at[mid], relay, relay_send, relay_recv, group - quarter)
    second_leg = remote(relay, recv[mid], data_send.at[mid], data_recv.at[mid], group - quarter)

    def pack(k, target, at):
        base = lax.rem(me + k, group) * slots

        def tile(t, carry):
            for i in range(8):
                j = t * 8 + i
                a = idx_ref[base + j]
                b = idx_ref[base + half + j]
                row = jnp.where(left, score[pl.ds(a, 1), :], score[pl.ds(b, 1), :])
                if at is None:
                    target[pl.ds(j, 1), :] = row
                else:
                    target[at, pl.ds(j, 1), :] = row
            return carry

        lax.fori_loop(0, half // 8, tile, 0)

    for k in range(1, group):
        cols_copy(k).start()
        offs_copy(k).start()
    order = [mid]
    for k in range(1, mid):
        order += [mid - k, mid + k]
    waiting = None
    for k in order:
        pack(k, send, k)
        if waiting is not None:
            waiting.start()
        waiting = first_leg if k == mid else data_copy(k)
    pack(0, recv[0], None)
    waiting.start()
    for k in range(1, group):
        knn_copy(k).start()
    own = [
        pltpu.make_async_copy(col_ref.at[me], rcol.at[0], own_sem.at[0]),
        pltpu.make_async_copy(off_ref.at[me], roff.at[0], own_sem.at[1]),
        pltpu.make_async_copy(knn_stat, rknn.at[0], own_sem.at[2]),
    ]
    for copy in own:
        copy.start()
    first_leg.wait()
    second_leg.start()

    def head_tile(tile, where):
        tile = jnp.dot(tile, turned[...], preferred_element_type=jnp.float32)
        logit[where, :] = tile
        return tile

    rest_copy = pltpu.make_async_copy(
        head_hbm.at[pl.ds(head_full * HEAD_TILE, head_rest), :],
        head_buf.at[HEAD_BUFS, pl.ds(0, head_rest), :],
        head_sem.at[HEAD_BUFS],
    )
    if head_rest:
        rest_copy.start()

    def head_step(step, total):
        @pl.when(step + HEAD_BUFS - 1 < head_full)
        def _():
            head_copy(step + HEAD_BUFS - 1).start()

        head_copy(step).wait()
        where = pl.ds(pl.multiple_of(step * HEAD_TILE, HEAD_TILE), HEAD_TILE)
        return merge(total, head_tile(head_buf[lax.rem(step, HEAD_BUFS)], where))

    total = lax.fori_loop(0, head_full, head_step, empty)
    if head_rest:
        rest_copy.wait()
        where = pl.ds(head_full * HEAD_TILE, head_rest)
        total = merge(total, head_tile(head_buf[HEAD_BUFS, :head_rest, :], where))
    lm_stat[0:1, :] = total[0]
    lm_stat[1:2, :] = total[1]
    lm_stat[2:8, :] = jnp.zeros((6, LANES), jnp.float32)
    hist[...] = jnp.zeros_like(hist)
    for pieces in (piece_a, piece_b):
        pieces[:, 2 * half :, :] = jnp.zeros((BATCH, WINDOW, LANES), jnp.float32)
    own.append(pltpu.make_async_copy(lm_stat, rlm.at[0], own_sem.at[3]))
    own[-1].start()
    for k in range(1, group):
        lm_copy(k).start()

    def combine(stat):
        top = stat[0, 0:1, :]
        for k in range(1, group):
            top = jnp.maximum(top, stat[k, 0:1, :])
        acc = jnp.zeros((1, LANES), jnp.float32)
        for k in range(group):
            acc = acc + stat[k, 1:2, :] * jnp.exp(stat[k, 0:1, :] - top)
        return top, acc

    for copy in own:
        copy.wait()
    for k in range(1, group):
        cols_copy(k).wait()
        offs_copy(k).wait()
        knn_copy(k).wait()
    to_smem = pltpu.make_async_copy(roff, off_smem, own_sem.at[0])
    to_smem.start()
    knn_max, knn_sum = combine(rknn)
    over = rknn[0, 2:3, :]
    for k in range(1, group):
        over = jnp.maximum(over, rknn[k, 2:3, :])
    to_smem.wait()

    lane = lax.broadcasted_iota(jnp.int32, (1, LANES), 1)
    column = lax.broadcasted_iota(jnp.int32, (COLS, LANES), 0)

    def split(where_i, start, value):
        high = value.astype(jnp.bfloat16).astype(jnp.float32)
        rest = value - high
        middle = rest.astype(jnp.bfloat16).astype(jnp.float32)
        piece_a[where_i, pl.ds(start, 8), :] = jnp.where(left, high, middle)
        piece_b[where_i, pl.ds(start, 8), :] = rest - middle

    def add_batch(members):
        for i, k in enumerate(members):

            def unpack(t, carry):
                start = pl.multiple_of(t * 8, 8)
                value = jnp.exp(recv[k][pl.ds(start, 8), :] - knn_max)
                other = pltpu.roll(value, LANES // 2, 1)
                split(i, start, jnp.where(left, value, other))
                split(i, pl.multiple_of(half + start, 8), jnp.where(left, other, value))
                return carry

            lax.fori_loop(0, half // 8, unpack, 0)

        def one_group(g, carry):
            values, hots = [], []
            pair = []
            for i, k in enumerate(members):
                start = off_smem[k, 0, g]
                values.append(
                    jnp.concatenate(
                        [
                            piece_a[i, pl.ds(start, WINDOW), :].astype(jnp.bfloat16),
                            piece_b[i, pl.ds(start, WINDOW), :].astype(jnp.bfloat16),
                        ],
                        axis=1,
                    )
                )
                row, off = start // LANES, start % LANES
                low = rcol[k, pl.ds(row, 1), :]
                high = rcol[k, pl.ds(jnp.minimum(row + 1, rows - 1), 1), :]
                shift = (2 * LANES - off + WINDOW * (i % 2)) % LANES
                seen = jnp.where(lane < off, high, low)
                pair.append(pltpu.roll(seen, shift, 1))
                if i % 2:
                    cols = jnp.where(left, pair[i - 1], pair[i]) - g * COLS
                    hots.append(jnp.where(column == cols, 1.0, 0.0).astype(jnp.bfloat16))
            part = jnp.dot(
                jnp.concatenate(hots, axis=1), jnp.concatenate(values, axis=0),
                preferred_element_type=jnp.float32,
            )
            where = pl.ds(pl.multiple_of(g * COLS, COLS), COLS)
            both = part[:, :LANES]
            hist[where, :] += both + pltpu.roll(both, LANES // 2, 1) + part[:, LANES:]
            return carry

        lax.fori_loop(0, hist.shape[0] // COLS, one_group, 0, unroll=2)

    queue = [0] + [k for k in order if k != mid]
    queue.insert(max(len(queue) - BATCH, 1), mid)
    for at in range(0, group, BATCH):
        members = queue[at : at + BATCH]
        for k in members:
            if k == mid:
                second_leg.wait()
            elif k:
                data_copy(k).wait()
        add_batch(members)

    for k in range(1, group):
        lm_copy(k).wait()
    lm_max, lm_sum = combine(rlm)
    sum_ref[0:1, :] = knn_max
    sum_ref[1:2, :] = knn_sum
    sum_ref[2:3, :] = lm_max
    sum_ref[3:4, :] = lm_sum
    sum_ref[4:8, :] = jnp.broadcast_to(over, (4, LANES))

    mix = mix_ref[0]
    knn_scale = mix / knn_sum
    lm_scale = (1.0 - mix) / lm_sum

    def tile(start, count):
        where = pl.ds(start, count)
        prob = hist[where, :] * knn_scale + jnp.exp(logit[where, :] - lm_max) * lm_scale
        return jnp.log(prob)

    full = vocab // LANES

    def write(i, carry):
        start = pl.multiple_of(i * LANES, LANES)
        out_ref[:, pl.ds(start, LANES)] = tile(start, LANES).T[: LANES // 2, :]
        return carry

    lax.fori_loop(0, full, write, 0)
    rest = vocab - full * LANES
    if rest:
        last = jnp.concatenate(
            [tile(full * LANES, rest), jnp.zeros((LANES - rest, LANES), jnp.float32)], axis=0
        )
        out_ref[:, full * LANES :] = last.T[: LANES // 2, :rest]


def solution(mesh):
    group = mesh.shape["model"]

    def local_step(queries, w_shard, key_shard, tok_shard, temperature, mix_weight):
        row_count, depth = queries.shape
        vocab, n_local = w_shard.shape[1], key_shard.shape[0]
        mean = n_local / group
        cap = round_up(int(mean + 4.5 * math.sqrt(mean)), 16)
        half = cap // 2
        slot_rows = round_up(cap, LANES) // LANES
        slots = slot_rows * LANES
        groups = round_up(vocab, 2 * COLS) // COLS

        order_tok, order_idx = lax.sort(
            (tok_shard, lax.iota(jnp.int32, n_local)), num_keys=1, is_stable=False
        )
        pad = (slot_rows + 8) * LANES
        fill = jnp.zeros((pad,), jnp.int32)
        shape_2d = ((n_local + pad) // LANES, LANES)
        tok_2d = jnp.concatenate([order_tok, fill]).reshape(shape_2d)
        idx_2d = jnp.concatenate([order_idx, fill]).reshape(shape_2d)

        smem = pl.BlockSpec(memory_space=pltpu.SMEM)
        vmem = pl.BlockSpec(memory_space=pltpu.VMEM)
        hbm = pl.BlockSpec(memory_space=pl.ANY)
        cols, idx, offs, over = pl.pallas_call(
            functools.partial(slot_kernel, group, vocab, cap, slot_rows, n_local),
            out_shape=(
                jax.ShapeDtypeStruct((group, slot_rows, LANES), jnp.int32),
                jax.ShapeDtypeStruct((group * slot_rows, LANES), jnp.int32),
                jax.ShapeDtypeStruct((group, 1, LANES), jnp.int32),
                jax.ShapeDtypeStruct((8, LANES), jnp.float32),
            ),
            in_specs=[vmem, vmem],
            out_specs=(vmem, vmem, vmem, vmem),
            name="slots",
        )(tok_2d, idx_2d)

        stat = pltpu.VMEM((8, LANES), jnp.float32)
        stats = pltpu.VMEM((group, 8, LANES), jnp.float32)
        pieces = pltpu.VMEM((BATCH, 2 * half + WINDOW, LANES), jnp.float32)
        dma = pltpu.SemaphoreType.DMA
        chunk = pltpu.VMEM((half, LANES), jnp.float32)
        fast, sums = pl.pallas_call(
            functools.partial(exchange_kernel, group, half, slot_rows),
            out_shape=(
                jax.ShapeDtypeStruct((row_count, vocab), jnp.float32),
                jax.ShapeDtypeStruct((8, LANES), jnp.float32),
            ),
            in_specs=[smem, smem, smem, vmem, vmem, vmem, vmem, hbm, hbm],
            out_specs=(vmem, vmem),
            scratch_shapes=[
                pltpu.VMEM((KEY_BUFS, KEY_TILE, depth), jnp.bfloat16),
                pltpu.VMEM((HEAD_BUFS + 1, HEAD_TILE, depth), jnp.bfloat16),
                pltpu.VMEM((depth, LANES), jnp.bfloat16),
                pltpu.VMEM((n_local, LANES), jnp.float32),
                pltpu.VMEM((group, half, LANES), jnp.float32),
                chunk,
                [chunk] * group,
                pltpu.VMEM((group, slot_rows, LANES), jnp.int32),
                pltpu.VMEM((group, 1, LANES), jnp.int32),
                pltpu.SMEM((group, 1, LANES), jnp.int32),
                stat, stat, stats, stats,
                pltpu.VMEM((vocab, LANES), jnp.float32),
                pltpu.VMEM((groups * COLS, LANES), jnp.float32),
                pieces, pieces,
                dma((KEY_BUFS,)), dma((HEAD_BUFS + 1,)), dma((group,)), dma((group,)), dma, dma,
                dma((group,)), dma((group,)), dma((group,)), dma((group,)),
                dma((group,)), dma((group,)), dma((group,)), dma((group,)), dma((4,)),
            ],
            compiler_params=pltpu.CompilerParams(
                collective_id=0, has_side_effects=True, vmem_limit_bytes=VMEM_LIMIT
            ),
            name="exchange",
        )(idx.reshape(-1), temperature, mix_weight, queries, over, cols, offs, key_shard, w_shard.T)

        def dense(unused):
            me = lax.axis_index("model")
            row_max, row_total = sums[0, :row_count], sums[1, :row_count]
            lm_max, lm_total = sums[2, :row_count], sums[3, :row_count]
            cross_dot = jnp.einsum("bd,nd->nb", queries, key_shard, preferred_element_type=jnp.float32)
            key_sq = jnp.sum(jnp.square(key_shard.astype(jnp.float32)), axis=1)
            scores = (2.0 * cross_dot - key_sq[:, None]) / temperature[0]
            weights = jnp.exp(scores - row_max[None, :])
            ring = [(i, (i + 1) % group) for i in range(group)]

            def turn(k, acc):
                acc = lax.ppermute(acc, "model", ring)
                col = tok_shard - lax.rem(me + group - 1 - k, group) * vocab
                col = jnp.where((col >= 0) & (col < vocab), col, vocab)
                return acc.at[col].add(weights)

            acc = jnp.zeros((vocab + 1, row_count), jnp.float32)
            acc = lax.fori_loop(0, group, turn, acc)
            logit = jnp.dot(queries, w_shard, preferred_element_type=jnp.float32)
            p_lm = jnp.exp(logit - lm_max[:, None]) / lm_total[:, None]
            p_knn = acc[:vocab].T / row_total[:, None]
            mix_value = mix_weight[0]
            return jnp.log(mix_value * p_knn + (1.0 - mix_value) * p_lm)

        return lax.cond(sums[4, 0] > 0.0, dense, lambda kept: kept, fast)

    return jax.shard_map(
        local_step,
        mesh=mesh,
        in_specs=(P("data", None), P(None, "model"), P("model", None), P("model"), P(), P()),
        out_specs=P("data", "model"),
        check_vma=False,
    )
```

```python
import functools
import math

import jax
import jax.numpy as jnp
from jax import lax
from jax.experimental import pallas as pl
from jax.experimental.pallas import tpu as pltpu
from jax.sharding import PartitionSpec as P

MESH = pl.DeviceIdType.MESH
LANES = 128
KEY_TILE = 512
KEY_BUFS = 4
HEAD_TILE = 512
HEAD_BUFS = 3
COLS = 256
WINDOW = 64
BATCH = 4
VMEM_LIMIT = 60 * 1024 * 1024


def round_up(value, step):
    return (value + step - 1) // step * step


def slot_kernel(group, vocab, cap, rows, n_local, tok_ref, ord_ref, col_ref, idx_ref, over_ref):
    lane = lax.broadcasted_iota(jnp.int32, (rows, LANES), 1)
    slot = lax.broadcasted_iota(jnp.int32, (rows, LANES), 0) * LANES + lane
    bound = lax.broadcasted_iota(jnp.int32, (LANES, LANES), 0)
    across = lax.broadcasted_iota(jnp.int32, (LANES, LANES), 1)
    tokens = tok_ref[: n_local // LANES, :]

    def below(limit):
        return jnp.sum((tokens < limit).astype(jnp.int32))

    starts = [0] + [below(d * vocab) for d in range(1, group)] + [n_local]
    table = jnp.zeros((LANES, LANES), jnp.float32)
    most = jnp.int32(0)
    for d in range(group):
        start, count = starts[d], starts[d + 1] - starts[d]
        most = jnp.maximum(most, count)
        row, off = start // LANES, start % LANES
        shift = (LANES - off) % LANES

        def shifted(ref):
            low = pltpu.roll(ref[pl.ds(row, rows), :], shift, 1)
            high = pltpu.roll(ref[pl.ds(row + 1, rows), :], shift, 1)
            return jnp.where(lane < LANES - off, low, high)

        used = slot < count
        col = jnp.where(used, shifted(tok_ref) - d * vocab, vocab)
        col_ref[d, :rows, :] = col
        idx_ref[d * rows : (d + 1) * rows, :] = jnp.where(used, shifted(ord_ref), 0)
        first = jnp.where(used, col // COLS, LANES)
        hits = jnp.zeros((LANES, LANES), jnp.float32)
        for r in range(rows):
            hits = hits + jnp.where(first[r : r + 1, :] < bound, 1.0, 0.0)
        table = jnp.where(across == d, jnp.sum(hits, axis=1, keepdims=True), table)
    widest = jnp.max(table[1:, :] - table[:-1, :])
    over = jnp.where((most > cap) | (widest > WINDOW), 1.0, 0.0)
    over_ref[...] = jnp.full((8, LANES), over, jnp.float32)
    turned = jnp.minimum(table, float(cap)).T.astype(jnp.int32)
    for d in range(group):
        col_ref[d, rows : rows + 1, :] = turned[d : d + 1, :]


def exchange_kernel(
    group, half, rows, idx_ref, temp_ref, query_ref, over_ref, col_ref, key_hbm, head_hbm,
    recv_hbm, rcol_hbm, rstat_hbm, logit_hbm,
    key_buf, head_buf, turned, score, send, relay, stat, logit,
    key_sem, head_sem, data_send, data_recv, relay_send, relay_recv, col_send, col_recv,
    stat_send, stat_recv, own_sem,
):
    me = lax.axis_index("model")
    n_local, vocab = key_hbm.shape[0], head_hbm.shape[0]
    slots = rows * LANES
    mid, quarter = group // 2, group // 4

    def peer(k):
        return {"model": lax.rem(me + k, group)}

    barrier = pltpu.get_barrier_semaphore()
    for k in range(1, group):
        pl.semaphore_signal(barrier, inc=1, device_id=peer(k), device_id_type=MESH)

    def key_copy(step):
        return pltpu.make_async_copy(
            key_hbm.at[pl.ds(step * KEY_TILE, KEY_TILE), :],
            key_buf.at[lax.rem(step, KEY_BUFS)],
            key_sem.at[lax.rem(step, KEY_BUFS)],
        )

    head_full = vocab // HEAD_TILE
    head_rest = vocab - head_full * HEAD_TILE

    def head_copy(step):
        return pltpu.make_async_copy(
            head_hbm.at[pl.ds(step * HEAD_TILE, HEAD_TILE), :],
            head_buf.at[lax.rem(step, HEAD_BUFS)],
            head_sem.at[lax.rem(step, HEAD_BUFS)],
        )

    key_steps = n_local // KEY_TILE
    for step in range(KEY_BUFS - 1):
        key_copy(step).start()

    temp = temp_ref[0]
    query = query_ref[...].astype(jnp.float32)
    turned[...] = jnp.concatenate([query, query], axis=0).T.astype(jnp.bfloat16)

    def merge(total, tile):
        top, acc = total
        new = jnp.maximum(top, jnp.max(tile, axis=0, keepdims=True))
        acc = acc * jnp.exp(top - new) + jnp.sum(jnp.exp(tile - new), axis=0, keepdims=True)
        return new, acc

    empty = (jnp.full((1, LANES), -3e38, jnp.float32), jnp.zeros((1, LANES), jnp.float32))

    def score_step(step, total):
        @pl.when(step + KEY_BUFS - 1 < key_steps)
        def _():
            key_copy(step + KEY_BUFS - 1).start()

        key_copy(step).wait()
        keys = key_buf[lax.rem(step, KEY_BUFS)]
        cross = jnp.dot(keys, turned[...], preferred_element_type=jnp.float32)
        wide = keys.astype(jnp.float32)
        square = jnp.sum(wide * wide, axis=1, keepdims=True)
        tile = (2.0 * cross - square) / temp
        score[pl.ds(pl.multiple_of(step * KEY_TILE, KEY_TILE), KEY_TILE), :] = tile
        return merge(total, tile)

    knn_max, knn_sum = lax.fori_loop(0, key_steps, score_step, empty)

    for step in range(HEAD_BUFS - 1):
        head_copy(step).start()

    pl.semaphore_wait(barrier, group - 1)

    left = lax.broadcasted_iota(jnp.int32, (1, LANES), 1) < LANES // 2

    def remote(src, dst, send_sem, recv_sem, k):
        return pltpu.make_async_remote_copy(
            src_ref=src, dst_ref=dst, send_sem=send_sem, recv_sem=recv_sem,
            device_id=peer(k), device_id_type=MESH,
        )

    def data_copy(k):
        return remote(send.at[k], recv_hbm.at[k], data_send.at[k], data_recv.at[k], k)

    def cols_copy(k):
        return remote(col_ref.at[lax.rem(me + k, group)], rcol_hbm.at[k], col_send.at[k], col_recv.at[k], k)

    def stat_copy(k):
        return remote(stat, rstat_hbm.at[k], stat_send.at[k], stat_recv.at[k], k)

    first_leg = remote(send.at[mid], relay, relay_send, relay_recv, group - quarter)
    second_leg = remote(relay, recv_hbm.at[mid], data_send.at[mid], data_recv.at[mid], group - quarter)

    def pack(k):
        base = lax.rem(me + k, group) * slots

        def tile(t, carry):
            for i in range(8):
                j = t * 8 + i
                a = idx_ref[base + j]
                b = idx_ref[base + half + j]
                row = jnp.where(left, score[pl.ds(a, 1), :], score[pl.ds(b, 1), :])
                send[k, pl.ds(j, 1), :] = row
            return carry

        lax.fori_loop(0, half // 8, tile, 0)

    for k in range(1, group):
        cols_copy(k).start()
    order = [mid]
    for k in range(1, mid):
        order += [mid - k, mid + k]
    waiting = None
    for k in order:
        pack(k)
        if waiting is not None:
            waiting.start()
        waiting = first_leg if k == mid else data_copy(k)
    pack(0)
    waiting.start()
    first_leg.wait()
    second_leg.start()

    def head_tile(tile, where):
        tile = jnp.dot(tile, turned[...], preferred_element_type=jnp.float32)
        logit[where, :] = tile
        return tile

    rest_copy = pltpu.make_async_copy(
        head_hbm.at[pl.ds(head_full * HEAD_TILE, head_rest), :],
        head_buf.at[HEAD_BUFS, pl.ds(0, head_rest), :],
        head_sem.at[HEAD_BUFS],
    )
    if head_rest:
        rest_copy.start()

    def head_step(step, total):
        @pl.when(step + HEAD_BUFS - 1 < head_full)
        def _():
            head_copy(step + HEAD_BUFS - 1).start()

        head_copy(step).wait()
        where = pl.ds(pl.multiple_of(step * HEAD_TILE, HEAD_TILE), HEAD_TILE)
        return merge(total, head_tile(head_buf[lax.rem(step, HEAD_BUFS)], where))

    total = lax.fori_loop(0, head_full, head_step, empty)
    if head_rest:
        rest_copy.wait()
        where = pl.ds(head_full * HEAD_TILE, head_rest)
        total = merge(total, head_tile(head_buf[HEAD_BUFS, :head_rest, :], where))

    stat[0:1, :] = knn_max
    stat[1:2, :] = knn_sum
    stat[2:3, :] = total[0]
    stat[3:4, :] = total[1]
    stat[4:8, :] = over_ref[4:8, :]
    own = [
        pltpu.make_async_copy(send.at[0], recv_hbm.at[0], own_sem.at[0]),
        pltpu.make_async_copy(col_ref.at[me], rcol_hbm.at[0], own_sem.at[1]),
        pltpu.make_async_copy(logit, logit_hbm, own_sem.at[2]),
        pltpu.make_async_copy(stat, rstat_hbm.at[0], own_sem.at[3]),
    ]
    for copy in own:
        copy.start()
    for k in range(1, group):
        stat_copy(k).start()
    for copy in own:
        copy.wait()
    for k in range(1, group):
        stat_copy(k).wait()
        cols_copy(k).wait()
        if k == mid:
            second_leg.wait()
        else:
            data_copy(k).wait()


def finish_kernel(
    group, half, rows, off_smem, mix_ref, rcol, stat, recv_hbm, logit_hbm, out_ref, sum_ref,
    recv, logit, hist, piece_a, piece_b, recv_sem, logit_sem,
):
    vocab = logit_hbm.shape[0]
    batches = group // BATCH

    def fetch(b):
        where = pl.ds(b * BATCH, BATCH)
        return pltpu.make_async_copy(recv_hbm.at[where], recv.at[where], recv_sem.at[b])

    for b in range(batches):
        fetch(b).start()
    fetch_logit = pltpu.make_async_copy(logit_hbm, logit, logit_sem)
    fetch_logit.start()

    def combine(row):
        top = stat[0, row : row + 1, :]
        for k in range(1, group):
            top = jnp.maximum(top, stat[k, row : row + 1, :])
        acc = jnp.zeros((1, LANES), jnp.float32)
        for k in range(group):
            acc = acc + stat[k, row + 1 : row + 2, :] * jnp.exp(stat[k, row : row + 1, :] - top)
        return top, acc

    knn_max, knn_sum = combine(0)
    lm_max, lm_sum = combine(2)
    over = stat[0, 4:5, :]
    for k in range(1, group):
        over = jnp.maximum(over, stat[k, 4:5, :])
    sum_ref[0:1, :] = knn_max
    sum_ref[1:2, :] = knn_sum
    sum_ref[2:3, :] = lm_max
    sum_ref[3:4, :] = lm_sum
    sum_ref[4:8, :] = jnp.broadcast_to(over, (4, LANES))

    hist[...] = jnp.zeros_like(hist)
    for pieces in (piece_a, piece_b):
        pieces[:, 2 * half :, :] = jnp.zeros((BATCH, WINDOW, LANES), jnp.float32)

    lane = lax.broadcasted_iota(jnp.int32, (1, LANES), 1)
    left = lane < LANES // 2
    column = lax.broadcasted_iota(jnp.int32, (COLS, LANES), 0)

    def split(i, start, count, value):
        high = value.astype(jnp.bfloat16).astype(jnp.float32)
        rest = value - high
        middle = rest.astype(jnp.bfloat16).astype(jnp.float32)
        piece_a[i, pl.ds(start, count), :] = jnp.where(left, high, middle)
        piece_b[i, pl.ds(start, count), :] = rest - middle

    def one_batch(b, carry):
        fetch(b).wait()
        for i in range(BATCH):

            def unpack(t, carry):
                start = pl.multiple_of(t * 8, 8)
                value = jnp.exp(recv[b * BATCH + i, pl.ds(start, 8), :] - knn_max)
                other = pltpu.roll(value, LANES // 2, 1)
                split(i, start, 8, jnp.where(left, value, other))
                split(i, pl.multiple_of(half + start, 8), 8, jnp.where(left, other, value))
                return carry

            lax.fori_loop(0, half // 8, unpack, 0, unroll=4)

        def one_group(g, carry):
            values, hots = [], []
            pair = []
            for i in range(BATCH):
                k = b * BATCH + i
                start = off_smem[k * LANES + g]
                values.append(
                    jnp.concatenate(
                        [
                            piece_a[i, pl.ds(start, WINDOW), :].astype(jnp.bfloat16),
                            piece_b[i, pl.ds(start, WINDOW), :].astype(jnp.bfloat16),
                        ],
                        axis=1,
                    )
                )
                row, off = start // LANES, start % LANES
                low = rcol[k, pl.ds(row, 1), :]
                high = rcol[k, pl.ds(jnp.minimum(row + 1, rows - 1), 1), :]
                shift = (2 * LANES - off + WINDOW * (i % 2)) % LANES
                seen = jnp.where(lane < off, high, low)
                pair.append(pltpu.roll(seen, shift, 1))
                if i % 2:
                    cols = jnp.where(left, pair[i - 1], pair[i]) - g * COLS
                    hots.append(jnp.where(column == cols, 1.0, 0.0).astype(jnp.bfloat16))
            part = jnp.dot(
                jnp.concatenate(hots, axis=1), jnp.concatenate(values, axis=0),
                preferred_element_type=jnp.float32,
            )
            where = pl.ds(pl.multiple_of(g * COLS, COLS), COLS)
            both = part[:, :LANES]
            hist[where, :] += both + pltpu.roll(both, LANES // 2, 1) + part[:, LANES:]
            return carry

        lax.fori_loop(0, hist.shape[0] // COLS, one_group, 0, unroll=2)
        return carry

    lax.fori_loop(0, batches, one_batch, 0)
    fetch_logit.wait()

    mix = mix_ref[0]
    knn_scale = mix / knn_sum
    lm_scale = (1.0 - mix) / lm_sum

    def tile(start, count):
        where = pl.ds(start, count)
        prob = hist[where, :] * knn_scale + jnp.exp(logit[where, :] - lm_max) * lm_scale
        return jnp.log(prob)

    full = vocab // LANES

    def write(i, carry):
        start = pl.multiple_of(i * LANES, LANES)
        out_ref[:, pl.ds(start, LANES)] = tile(start, LANES).T[: LANES // 2, :]
        return carry

    lax.fori_loop(0, full, write, 0)
    rest = vocab - full * LANES
    if rest:
        last = jnp.concatenate(
            [tile(full * LANES, rest), jnp.zeros((LANES - rest, LANES), jnp.float32)], axis=0
        )
        out_ref[:, full * LANES :] = last.T[: LANES // 2, :rest]


def solution(mesh):
    group = mesh.shape["model"]

    def local_step(queries, w_shard, key_shard, tok_shard, temperature, mix_weight):
        row_count, depth = queries.shape
        vocab, n_local = w_shard.shape[1], key_shard.shape[0]
        mean = n_local / group
        cap = round_up(int(mean + 4.5 * math.sqrt(mean)), 16)
        half = cap // 2
        slot_rows = round_up(cap, LANES) // LANES
        slots = slot_rows * LANES
        groups = round_up(vocab, 2 * COLS) // COLS

        order_tok, order_idx = lax.sort(
            (tok_shard, lax.iota(jnp.int32, n_local)), num_keys=1, is_stable=False
        )
        pad = (slot_rows + 8) * LANES
        fill = jnp.zeros((pad,), jnp.int32)
        shape_2d = ((n_local + pad) // LANES, LANES)
        tok_2d = jnp.concatenate([order_tok, fill]).reshape(shape_2d)
        idx_2d = jnp.concatenate([order_idx, fill]).reshape(shape_2d)

        smem = pl.BlockSpec(memory_space=pltpu.SMEM)
        vmem = pl.BlockSpec(memory_space=pltpu.VMEM)
        hbm = pl.BlockSpec(memory_space=pl.ANY)
        table = jax.ShapeDtypeStruct((group, slot_rows + 1, LANES), jnp.int32)
        cols, idx, over = pl.pallas_call(
            functools.partial(slot_kernel, group, vocab, cap, slot_rows, n_local),
            out_shape=(
                table,
                jax.ShapeDtypeStruct((group * slot_rows, LANES), jnp.int32),
                jax.ShapeDtypeStruct((8, LANES), jnp.float32),
            ),
            in_specs=[vmem, vmem],
            out_specs=(vmem, vmem, vmem),
            name="slots",
        )(tok_2d, idx_2d)

        dma = pltpu.SemaphoreType.DMA
        chunk = pltpu.VMEM((half, LANES), jnp.float32)
        logit = pltpu.VMEM((vocab, LANES), jnp.float32)
        recv, rcols, rstat, logits = pl.pallas_call(
            functools.partial(exchange_kernel, group, half, slot_rows),
            out_shape=(
                jax.ShapeDtypeStruct((group, half, LANES), jnp.float32),
                table,
                jax.ShapeDtypeStruct((group, 8, LANES), jnp.float32),
                jax.ShapeDtypeStruct((vocab, LANES), jnp.float32),
            ),
            in_specs=[smem, smem, vmem, vmem, vmem, hbm, hbm],
            out_specs=(hbm, hbm, hbm, hbm),
            scratch_shapes=[
                pltpu.VMEM((KEY_BUFS, KEY_TILE, depth), jnp.bfloat16),
                pltpu.VMEM((HEAD_BUFS + 1, HEAD_TILE, depth), jnp.bfloat16),
                pltpu.VMEM((depth, LANES), jnp.bfloat16),
                pltpu.VMEM((n_local, LANES), jnp.float32),
                pltpu.VMEM((group, half, LANES), jnp.float32),
                chunk,
                pltpu.VMEM((8, LANES), jnp.float32),
                logit,
                dma((KEY_BUFS,)), dma((HEAD_BUFS + 1,)), dma((group,)), dma((group,)), dma, dma,
                dma((group,)), dma((group,)), dma((group,)), dma((group,)), dma((4,)),
            ],
            compiler_params=pltpu.CompilerParams(
                collective_id=0, has_side_effects=True, vmem_limit_bytes=VMEM_LIMIT
            ),
            name="exchange",
        )(idx.reshape(-1), temperature, queries, over, cols, key_shard, w_shard.T)

        pieces = pltpu.VMEM((BATCH, 2 * half + WINDOW, LANES), jnp.float32)
        fast, sums = pl.pallas_call(
            functools.partial(finish_kernel, group, half, slot_rows),
            out_shape=(
                jax.ShapeDtypeStruct((row_count, vocab), jnp.float32),
                jax.ShapeDtypeStruct((8, LANES), jnp.float32),
            ),
            in_specs=[smem, smem, vmem, vmem, hbm, hbm],
            out_specs=(vmem, vmem),
            scratch_shapes=[
                pltpu.VMEM((group, half, LANES), jnp.float32),
                logit,
                pltpu.VMEM((groups * COLS, LANES), jnp.float32),
                pieces, pieces, dma((group // BATCH,)), dma,
            ],
            compiler_params=pltpu.CompilerParams(vmem_limit_bytes=VMEM_LIMIT),
            name="finish",
        )(rcols[:, slot_rows, :].reshape(-1), mix_weight, rcols, rstat, recv, logits)

        def dense(unused):
            me = lax.axis_index("model")
            row_max, row_total = sums[0, :row_count], sums[1, :row_count]
            lm_max, lm_total = sums[2, :row_count], sums[3, :row_count]
            cross_dot = jnp.einsum("bd,nd->nb", queries, key_shard, preferred_element_type=jnp.float32)
            key_sq = jnp.sum(jnp.square(key_shard.astype(jnp.float32)), axis=1)
            scores = (2.0 * cross_dot - key_sq[:, None]) / temperature[0]
            weights = jnp.exp(scores - row_max[None, :])
            ring = [(i, (i + 1) % group) for i in range(group)]

            def turn(k, acc):
                acc = lax.ppermute(acc, "model", ring)
                col = tok_shard - lax.rem(me + group - 1 - k, group) * vocab
                col = jnp.where((col >= 0) & (col < vocab), col, vocab)
                return acc.at[col].add(weights)

            acc = jnp.zeros((vocab + 1, row_count), jnp.float32)
            acc = lax.fori_loop(0, group, turn, acc)
            logit = jnp.dot(queries, w_shard, preferred_element_type=jnp.float32)
            p_lm = jnp.exp(logit - lm_max[:, None]) / lm_total[:, None]
            p_knn = acc[:vocab].T / row_total[:, None]
            mix_value = mix_weight[0]
            return jnp.log(mix_value * p_knn + (1.0 - mix_value) * p_lm)

        return lax.cond(sums[4, 0] > 0.0, dense, lambda kept: kept, fast)

    return jax.shard_map(
        local_step,
        mesh=mesh,
        in_specs=(P("data", None), P(None, "model"), P("model", None), P("model"), P(), P()),
        out_specs=P("data", "model"),
        check_vma=False,
    )
```

```python
import functools
import math

import jax
import jax.numpy as jnp
from jax import lax
from jax.experimental import pallas as pl
from jax.experimental.pallas import tpu as pltpu
from jax.sharding import PartitionSpec as P

MESH = pl.DeviceIdType.MESH
LANES = 128
KEY_TILE = 512
KEY_BUFS = 4
HEAD_TILE = 512
HEAD_BUFS = 3
HISTS = 8
ROWS = 16
CLEAR = 216
VMEM_LIMIT = 60 * 1024 * 1024


def round_up(value, step):
    return (value + step - 1) // step * step


def slot_kernel(group, vocab, cap, rows, n_local, tok_ref, ord_ref, col_ref, idx_ref, over_ref):
    lane = lax.broadcasted_iota(jnp.int32, (rows, LANES), 1)
    slot = lax.broadcasted_iota(jnp.int32, (rows, LANES), 0) * LANES + lane
    tokens = tok_ref[: n_local // LANES, :]

    def below(limit):
        return jnp.sum((tokens < limit).astype(jnp.int32))

    starts = [0] + [below(d * vocab) for d in range(1, group)] + [n_local]
    most = jnp.int32(0)
    for d in range(group):
        start, count = starts[d], starts[d + 1] - starts[d]
        most = jnp.maximum(most, count)
        row, off = start // LANES, start % LANES
        shift = (LANES - off) % LANES

        def shifted(ref):
            low = pltpu.roll(ref[pl.ds(row, rows), :], shift, 1)
            high = pltpu.roll(ref[pl.ds(row + 1, rows), :], shift, 1)
            return jnp.where(lane < LANES - off, low, high)

        used = slot < count
        col_ref[d] = jnp.where(used, shifted(tok_ref) - d * vocab, vocab)
        idx_ref[d * rows : (d + 1) * rows, :] = jnp.where(used, shifted(ord_ref), 0)
    over = jnp.where(most > cap, 1.0, 0.0)
    over_ref[...] = jnp.full((8, LANES), over, jnp.float32)


def exchange_kernel(
    group, half, rows, idx_ref, temp_ref, query_ref, over_ref, col_ref, key_hbm, head_hbm,
    recv_hbm, rcol_hbm, rstat_hbm, logit_hbm,
    key_buf, head_buf, turned, score, send, stat, logit,
    key_sem, head_sem, data_send, data_recv, col_send, col_recv,
    stat_send, stat_recv, own_sem,
):
    me = lax.axis_index("model")
    n_local, vocab = key_hbm.shape[0], head_hbm.shape[0]
    slots = rows * LANES
    mid = group // 2

    def peer(k):
        return {"model": lax.rem(me + k, group)}

    barrier = pltpu.get_barrier_semaphore()
    for k in range(1, group):
        pl.semaphore_signal(barrier, inc=1, device_id=peer(k), device_id_type=MESH)

    def key_copy(step):
        return pltpu.make_async_copy(
            key_hbm.at[pl.ds(step * KEY_TILE, KEY_TILE), :],
            key_buf.at[lax.rem(step, KEY_BUFS)],
            key_sem.at[lax.rem(step, KEY_BUFS)],
        )

    head_full = vocab // HEAD_TILE
    head_rest = vocab - head_full * HEAD_TILE

    def head_copy(step):
        return pltpu.make_async_copy(
            head_hbm.at[pl.ds(step * HEAD_TILE, HEAD_TILE), :],
            head_buf.at[lax.rem(step, HEAD_BUFS)],
            head_sem.at[lax.rem(step, HEAD_BUFS)],
        )

    key_steps = n_local // KEY_TILE
    for step in range(KEY_BUFS - 1):
        key_copy(step).start()

    temp = temp_ref[0]
    query = query_ref[...].astype(jnp.float32)
    turned[...] = jnp.concatenate([query, query], axis=0).T.astype(jnp.bfloat16)

    def merge(total, tile):
        top, acc = total
        new = jnp.maximum(top, jnp.max(tile, axis=0, keepdims=True))
        acc = acc * jnp.exp(top - new) + jnp.sum(jnp.exp(tile - new), axis=0, keepdims=True)
        return new, acc

    empty = (jnp.full((1, LANES), -3e38, jnp.float32), jnp.zeros((1, LANES), jnp.float32))

    def score_step(step, total):
        @pl.when(step + KEY_BUFS - 1 < key_steps)
        def _():
            key_copy(step + KEY_BUFS - 1).start()

        key_copy(step).wait()
        keys = key_buf[lax.rem(step, KEY_BUFS)]
        cross = jnp.dot(keys, turned[...], preferred_element_type=jnp.float32)
        wide = keys.astype(jnp.float32)
        square = jnp.sum(wide * wide, axis=1, keepdims=True)
        tile = (2.0 * cross - square) / temp
        score[pl.ds(pl.multiple_of(step * KEY_TILE, KEY_TILE), KEY_TILE), :] = tile
        return merge(total, tile)

    knn_max, knn_sum = lax.fori_loop(0, key_steps, score_step, empty)

    for step in range(HEAD_BUFS - 1):
        head_copy(step).start()

    pl.semaphore_wait(barrier, group - 1)

    left = lax.broadcasted_iota(jnp.int32, (1, LANES), 1) < LANES // 2

    def remote(src, dst, send_sem, recv_sem, k):
        return pltpu.make_async_remote_copy(
            src_ref=src, dst_ref=dst, send_sem=send_sem, recv_sem=recv_sem,
            device_id=peer(k), device_id_type=MESH,
        )

    def data_copy(k):
        return remote(send.at[k], recv_hbm.at[k], data_send.at[k], data_recv.at[k], k)

    def cols_copy(k):
        return remote(col_ref.at[lax.rem(me + k, group)], rcol_hbm.at[k], col_send.at[k], col_recv.at[k], k)

    def stat_copy(k):
        return remote(stat, rstat_hbm.at[k], stat_send.at[k], stat_recv.at[k], k)

    def pack(k):
        base = lax.rem(me + k, group) * slots

        def tile(t, carry):
            for i in range(8):
                j = t * 8 + i
                a = idx_ref[base + j]
                b = idx_ref[base + half + j]
                row = jnp.where(left, score[pl.ds(a, 1), :], score[pl.ds(b, 1), :])
                send[k, pl.ds(j, 1), :] = row
            return carry

        lax.fori_loop(0, half // 8, tile, 0, unroll=2)

    for k in range(1, group):
        cols_copy(k).start()
    order = [mid]
    for k in range(1, mid):
        order += [mid - k, mid + k]
    waiting = None
    for k in order:
        pack(k)
        if waiting is not None:
            waiting.start()
        waiting = data_copy(k)
    pack(0)
    waiting.start()

    def head_tile(tile, where):
        tile = jnp.dot(tile, turned[...], preferred_element_type=jnp.float32)
        logit[where, :] = tile
        return tile

    rest_copy = pltpu.make_async_copy(
        head_hbm.at[pl.ds(head_full * HEAD_TILE, head_rest), :],
        head_buf.at[HEAD_BUFS, pl.ds(0, head_rest), :],
        head_sem.at[HEAD_BUFS],
    )
    if head_rest:
        rest_copy.start()

    def head_step(step, total):
        @pl.when(step + HEAD_BUFS - 1 < head_full)
        def _():
            head_copy(step + HEAD_BUFS - 1).start()

        head_copy(step).wait()
        where = pl.ds(pl.multiple_of(step * HEAD_TILE, HEAD_TILE), HEAD_TILE)
        return merge(total, head_tile(head_buf[lax.rem(step, HEAD_BUFS)], where))

    total = lax.fori_loop(0, head_full, head_step, empty)
    if head_rest:
        rest_copy.wait()
        where = pl.ds(head_full * HEAD_TILE, head_rest)
        total = merge(total, head_tile(head_buf[HEAD_BUFS, :head_rest, :], where))

    stat[0:1, :] = knn_max
    stat[1:2, :] = knn_sum
    stat[2:3, :] = total[0]
    stat[3:4, :] = total[1]
    stat[4:8, :] = over_ref[4:8, :]
    own = [
        pltpu.make_async_copy(send.at[0], recv_hbm.at[0], own_sem.at[0]),
        pltpu.make_async_copy(col_ref.at[me], rcol_hbm.at[0], own_sem.at[1]),
        pltpu.make_async_copy(logit, logit_hbm, own_sem.at[2]),
        pltpu.make_async_copy(stat, rstat_hbm.at[0], own_sem.at[3]),
    ]
    for copy in own:
        copy.start()
    for k in range(1, group):
        stat_copy(k).start()
    for copy in own:
        copy.wait()
    for k in range(1, group):
        stat_copy(k).wait()
        cols_copy(k).wait()
        data_copy(k).wait()


def finish_kernel(
    group, half, slots, col_ref, mix_ref, stat, recv_hbm, logit_hbm, out_ref, sum_ref,
    recv, logit, *rest_refs,
):
    hists, (recv_sem, logit_sem) = rest_refs[:HISTS], rest_refs[HISTS:]
    vocab = logit_hbm.shape[0]

    def fetch(d):
        return pltpu.make_async_copy(recv_hbm.at[d], recv.at[d], recv_sem.at[d])

    for d in range(group):
        fetch(d).start()
    fetch_logit = pltpu.make_async_copy(logit_hbm, logit, logit_sem)
    fetch_logit.start()

    def combine(row):
        top = stat[0, row : row + 1, :]
        for k in range(1, group):
            top = jnp.maximum(top, stat[k, row : row + 1, :])
        acc = jnp.zeros((1, LANES), jnp.float32)
        for k in range(group):
            acc = acc + stat[k, row + 1 : row + 2, :] * jnp.exp(stat[k, row : row + 1, :] - top)
        return top, acc

    knn_max, knn_sum = combine(0)
    lm_max, lm_sum = combine(2)
    over = stat[0, 4:5, :]
    for k in range(1, group):
        over = jnp.maximum(over, stat[k, 4:5, :])
    sum_ref[0:1, :] = knn_max
    sum_ref[1:2, :] = knn_sum
    sum_ref[2:3, :] = lm_max
    sum_ref[3:4, :] = lm_sum
    sum_ref[4:8, :] = jnp.broadcast_to(over, (4, LANES))

    def clear(i, carry):
        where = pl.ds(pl.multiple_of(i * CLEAR, CLEAR), CLEAR)
        for hist in hists:
            hist[where, :] = jnp.zeros((CLEAR, LANES), jnp.float32)
        return carry

    lax.fori_loop(0, hists[0].shape[0] // CLEAR, clear, 0)

    def one_source(d, carry):
        fetch(d).wait()
        recv[d] = jnp.exp(recv[d] - knn_max)

        def add_rows(j, count):
            base = d * slots + j
            for i in range(count):
                row = recv[d, pl.ds(j + i, 1), :]
                low = hists[2 * (i % (HISTS // 2))]
                high = hists[2 * (i % (HISTS // 2)) + 1]
                a = col_ref[base + i]
                low[pl.ds(a, 1), :] = low[pl.ds(a, 1), :] + row
                b = col_ref[base + half + i]
                high[pl.ds(b, 1), :] = high[pl.ds(b, 1), :] + row

        def step(t, carry):
            add_rows(t * ROWS, ROWS)
            return carry

        lax.fori_loop(0, half // ROWS, step, 0)
        if half % ROWS:
            add_rows(half // ROWS * ROWS, half % ROWS)
        return carry

    lax.fori_loop(0, group, one_source, 0)
    fetch_logit.wait()

    mix = mix_ref[0]
    knn_scale = mix / knn_sum
    lm_scale = (1.0 - mix) / lm_sum

    def tile(start, count):
        where = pl.ds(start, count)
        low, high = hists[0][where, :], hists[1][where, :]
        for hist in range(2, HISTS, 2):
            low = low + hists[hist][where, :]
            high = high + hists[hist + 1][where, :]
        hist = low + pltpu.roll(high, LANES // 2, 1)
        prob = hist * knn_scale + jnp.exp(logit[where, :] - lm_max) * lm_scale
        return jnp.log(prob)

    full = vocab // LANES

    def write(i, carry):
        start = pl.multiple_of(i * LANES, LANES)
        out_ref[:, pl.ds(start, LANES)] = tile(start, LANES).T[: LANES // 2, :]
        return carry

    lax.fori_loop(0, full, write, 0)
    rest = vocab - full * LANES
    if rest:
        last = jnp.concatenate(
            [tile(full * LANES, rest), jnp.zeros((LANES - rest, LANES), jnp.float32)], axis=0
        )
        out_ref[:, full * LANES :] = last.T[: LANES // 2, :rest]


def solution(mesh):
    group = mesh.shape["model"]

    def local_step(queries, w_shard, key_shard, tok_shard, temperature, mix_weight):
        row_count, depth = queries.shape
        vocab, n_local = w_shard.shape[1], key_shard.shape[0]
        mean = n_local / group
        cap = round_up(int(mean + 4.5 * math.sqrt(mean)), 16)
        half = cap // 2
        slot_rows = round_up(cap, LANES) // LANES
        slots = slot_rows * LANES

        order_tok, order_idx = lax.sort(
            (tok_shard, lax.iota(jnp.int32, n_local)), num_keys=1, is_stable=False
        )
        pad = (slot_rows + 8) * LANES
        fill = jnp.zeros((pad,), jnp.int32)
        shape_2d = ((n_local + pad) // LANES, LANES)
        tok_2d = jnp.concatenate([order_tok, fill]).reshape(shape_2d)
        idx_2d = jnp.concatenate([order_idx, fill]).reshape(shape_2d)

        smem = pl.BlockSpec(memory_space=pltpu.SMEM)
        vmem = pl.BlockSpec(memory_space=pltpu.VMEM)
        hbm = pl.BlockSpec(memory_space=pl.ANY)
        table = jax.ShapeDtypeStruct((group, slot_rows, LANES), jnp.int32)
        cols, idx, over = pl.pallas_call(
            functools.partial(slot_kernel, group, vocab, cap, slot_rows, n_local),
            out_shape=(
                table,
                jax.ShapeDtypeStruct((group * slot_rows, LANES), jnp.int32),
                jax.ShapeDtypeStruct((8, LANES), jnp.float32),
            ),
            in_specs=[vmem, vmem],
            out_specs=(vmem, vmem, vmem),
            name="slots",
        )(tok_2d, idx_2d)

        dma = pltpu.SemaphoreType.DMA
        logit = pltpu.VMEM((vocab, LANES), jnp.float32)
        recv, rcols, rstat, logits = pl.pallas_call(
            functools.partial(exchange_kernel, group, half, slot_rows),
            out_shape=(
                jax.ShapeDtypeStruct((group, half, LANES), jnp.float32),
                table,
                jax.ShapeDtypeStruct((group, 8, LANES), jnp.float32),
                jax.ShapeDtypeStruct((vocab, LANES), jnp.float32),
            ),
            in_specs=[smem, smem, vmem, vmem, vmem, hbm, hbm],
            out_specs=(hbm, hbm, hbm, hbm),
            scratch_shapes=[
                pltpu.VMEM((KEY_BUFS, KEY_TILE, depth), jnp.bfloat16),
                pltpu.VMEM((HEAD_BUFS + 1, HEAD_TILE, depth), jnp.bfloat16),
                pltpu.VMEM((depth, LANES), jnp.bfloat16),
                pltpu.VMEM((n_local, LANES), jnp.float32),
                pltpu.VMEM((group, half, LANES), jnp.float32),
                pltpu.VMEM((8, LANES), jnp.float32),
                logit,
                dma((KEY_BUFS,)), dma((HEAD_BUFS + 1,)), dma((group,)), dma((group,)),
                dma((group,)), dma((group,)), dma((group,)), dma((group,)), dma((4,)),
            ],
            compiler_params=pltpu.CompilerParams(
                collective_id=0, has_side_effects=True, vmem_limit_bytes=VMEM_LIMIT
            ),
            name="exchange",
        )(idx.reshape(-1), temperature, queries, over, cols, key_shard, w_shard.T)

        fast, sums = pl.pallas_call(
            functools.partial(finish_kernel, group, half, slots),
            out_shape=(
                jax.ShapeDtypeStruct((row_count, vocab), jnp.float32),
                jax.ShapeDtypeStruct((8, LANES), jnp.float32),
            ),
            in_specs=[smem, smem, vmem, hbm, hbm],
            out_specs=(vmem, vmem),
            scratch_shapes=[
                pltpu.VMEM((group, half, LANES), jnp.float32),
                logit,
                *[pltpu.VMEM((round_up(vocab + 1, CLEAR), LANES), jnp.float32)] * HISTS,
                dma((group,)), dma,
            ],
            compiler_params=pltpu.CompilerParams(vmem_limit_bytes=VMEM_LIMIT),
            name="finish",
        )(rcols.reshape(-1), mix_weight, rstat, recv, logits)

        def dense(unused):
            me = lax.axis_index("model")
            row_max, row_total = sums[0, :row_count], sums[1, :row_count]
            lm_max, lm_total = sums[2, :row_count], sums[3, :row_count]
            cross_dot = jnp.einsum("bd,nd->nb", queries, key_shard, preferred_element_type=jnp.float32)
            key_sq = jnp.sum(jnp.square(key_shard.astype(jnp.float32)), axis=1)
            scores = (2.0 * cross_dot - key_sq[:, None]) / temperature[0]
            weights = jnp.exp(scores - row_max[None, :])
            ring = [(i, (i + 1) % group) for i in range(group)]

            def turn(k, acc):
                acc = lax.ppermute(acc, "model", ring)
                col = tok_shard - lax.rem(me + group - 1 - k, group) * vocab
                col = jnp.where((col >= 0) & (col < vocab), col, vocab)
                return acc.at[col].add(weights)

            acc = jnp.zeros((vocab + 1, row_count), jnp.float32)
            acc = lax.fori_loop(0, group, turn, acc)
            logit = jnp.dot(queries, w_shard, preferred_element_type=jnp.float32)
            p_lm = jnp.exp(logit - lm_max[:, None]) / lm_total[:, None]
            p_knn = acc[:vocab].T / row_total[:, None]
            mix_value = mix_weight[0]
            return jnp.log(mix_value * p_knn + (1.0 - mix_value) * p_lm)

        return lax.cond(sums[4, 0] > 0.0, dense, lambda kept: kept, fast)

    return jax.shard_map(
        local_step,
        mesh=mesh,
        in_specs=(P("data", None), P(None, "model"), P("model", None), P("model"), P(), P()),
        out_specs=P("data", "model"),
        check_vma=False,
    )
```

```python
import functools
import math

import jax
import jax.numpy as jnp
from jax import lax
from jax.experimental import pallas as pl
from jax.experimental.pallas import tpu as pltpu
from jax.sharding import PartitionSpec as P

MESH = pl.DeviceIdType.MESH
LANES = 128
KEY_TILE = 512
KEY_BUFS = 4
HEAD_TILE = 512
HEAD_BUFS = 3
HISTS = 8
ROWS = 16
CLEAR = 216
VMEM_LIMIT = 60 * 1024 * 1024


def round_up(value, step):
    return (value + step - 1) // step * step


def slot_kernel(group, vocab, cap, rows, n_local, tok_ref, ord_ref, col_ref, idx_ref, over_ref):
    lane = lax.broadcasted_iota(jnp.int32, (rows, LANES), 1)
    slot = lax.broadcasted_iota(jnp.int32, (rows, LANES), 0) * LANES + lane
    tokens = tok_ref[: n_local // LANES, :]

    def below(limit):
        return jnp.sum((tokens < limit).astype(jnp.int32))

    starts = [0] + [below(d * vocab) for d in range(1, group)] + [n_local]
    most = jnp.int32(0)
    for d in range(group):
        start, count = starts[d], starts[d + 1] - starts[d]
        most = jnp.maximum(most, count)
        row, off = start // LANES, start % LANES
        shift = (LANES - off) % LANES

        def shifted(ref):
            low = pltpu.roll(ref[pl.ds(row, rows), :], shift, 1)
            high = pltpu.roll(ref[pl.ds(row + 1, rows), :], shift, 1)
            return jnp.where(lane < LANES - off, low, high)

        used = slot < count
        col_ref[d] = jnp.where(used, shifted(tok_ref) - d * vocab, vocab)
        idx_ref[d * rows : (d + 1) * rows, :] = jnp.where(used, shifted(ord_ref), 0)
    over = jnp.where(most > cap, 1.0, 0.0)
    over_ref[...] = jnp.full((8, LANES), over, jnp.float32)


def late_chunks(group):
    near = min(3, group // 2 - 1)
    return [k for k in range(1, group) if k <= near or k >= group - near]


def exchange_kernel(
    group, half, rows, idx_ref, temp_ref, query_ref, over_ref, col_ref, key_hbm, head_hbm,
    recv_hbm, rcol_hbm, rstat_hbm, logit_hbm, *refs,
):
    late = late_chunks(group)
    late_hbm, refs = refs[: len(late)], refs[len(late) :]
    (
        key_buf, head_buf, turned, score, send, stat, logit,
        key_sem, head_sem, data_send, data_recv, col_send, col_recv,
        stat_send, stat_recv, own_sem, late_sem,
    ) = refs
    me = lax.axis_index("model")
    n_local, vocab = key_hbm.shape[0], head_hbm.shape[0]
    slots = rows * LANES
    mid = group // 2

    def peer(k):
        return {"model": lax.rem(me + k, group)}

    barrier = pltpu.get_barrier_semaphore()
    for k in range(1, group):
        pl.semaphore_signal(barrier, inc=1, device_id=peer(k), device_id_type=MESH)

    def key_copy(step):
        return pltpu.make_async_copy(
            key_hbm.at[pl.ds(step * KEY_TILE, KEY_TILE), :],
            key_buf.at[lax.rem(step, KEY_BUFS)],
            key_sem.at[lax.rem(step, KEY_BUFS)],
        )

    head_full = vocab // HEAD_TILE
    head_rest = vocab - head_full * HEAD_TILE

    def head_copy(step):
        return pltpu.make_async_copy(
            head_hbm.at[pl.ds(step * HEAD_TILE, HEAD_TILE), :],
            head_buf.at[lax.rem(step, HEAD_BUFS)],
            head_sem.at[lax.rem(step, HEAD_BUFS)],
        )

    key_steps = n_local // KEY_TILE
    for step in range(KEY_BUFS - 1):
        key_copy(step).start()

    temp = temp_ref[0]
    query = query_ref[...].astype(jnp.float32)
    turned[...] = jnp.concatenate([query, query], axis=0).T.astype(jnp.bfloat16)

    def merge(total, tile):
        top, acc = total
        new = jnp.maximum(top, jnp.max(tile, axis=0, keepdims=True))
        acc = acc * jnp.exp(top - new) + jnp.sum(jnp.exp(tile - new), axis=0, keepdims=True)
        return new, acc

    empty = (jnp.full((1, LANES), -3e38, jnp.float32), jnp.zeros((1, LANES), jnp.float32))

    def score_step(step, total):
        @pl.when(step + KEY_BUFS - 1 < key_steps)
        def _():
            key_copy(step + KEY_BUFS - 1).start()

        key_copy(step).wait()
        keys = key_buf[lax.rem(step, KEY_BUFS)]
        cross = jnp.dot(keys, turned[...], preferred_element_type=jnp.float32)
        wide = keys.astype(jnp.float32)
        square = jnp.sum(wide * wide, axis=1, keepdims=True)
        tile = (2.0 * cross - square) / temp
        score[pl.ds(pl.multiple_of(step * KEY_TILE, KEY_TILE), KEY_TILE), :] = tile
        return merge(total, tile)

    knn_max, knn_sum = lax.fori_loop(0, key_steps, score_step, empty)

    for step in range(HEAD_BUFS - 1):
        head_copy(step).start()

    pl.semaphore_wait(barrier, group - 1)

    left = lax.broadcasted_iota(jnp.int32, (1, LANES), 1) < LANES // 2

    def remote(src, dst, send_sem, recv_sem, k):
        return pltpu.make_async_remote_copy(
            src_ref=src, dst_ref=dst, send_sem=send_sem, recv_sem=recv_sem,
            device_id=peer(k), device_id_type=MESH,
        )

    def data_copy(k):
        return remote(send.at[k], recv_hbm.at[k], data_send.at[k], data_recv.at[k], k)

    def cols_copy(k):
        return remote(col_ref.at[lax.rem(me + k, group)], rcol_hbm.at[k], col_send.at[k], col_recv.at[k], k)

    def stat_copy(k):
        return remote(stat, rstat_hbm.at[k], stat_send.at[k], stat_recv.at[k], k)

    def pack(k):
        base = lax.rem(me + k, group) * slots

        def tile(t, carry):
            for i in range(8):
                j = t * 8 + i
                a = idx_ref[base + j]
                b = idx_ref[base + half + j]
                row = jnp.where(left, score[pl.ds(a, 1), :], score[pl.ds(b, 1), :])
                send[k, pl.ds(j, 1), :] = row
            return carry

        lax.fori_loop(0, half // 8, tile, 0, unroll=2)

    for k in range(1, group):
        cols_copy(k).start()
    order = [mid]
    for k in range(1, mid):
        order += [mid - k, mid + k]
    waiting, handed = None, []
    for k in order:
        pack(k)
        if waiting is not None:
            waiting.start()
        if k in late:
            waiting = pltpu.make_async_copy(send.at[k], late_hbm[late.index(k)], late_sem.at[late.index(k)])
            handed.append(waiting)
        else:
            waiting = data_copy(k)
    pack(0)
    waiting.start()

    def head_tile(tile, where):
        tile = jnp.dot(tile, turned[...], preferred_element_type=jnp.float32)
        logit[where, :] = tile
        return tile

    rest_copy = pltpu.make_async_copy(
        head_hbm.at[pl.ds(head_full * HEAD_TILE, head_rest), :],
        head_buf.at[HEAD_BUFS, pl.ds(0, head_rest), :],
        head_sem.at[HEAD_BUFS],
    )
    if head_rest:
        rest_copy.start()

    def head_step(step, total):
        @pl.when(step + HEAD_BUFS - 1 < head_full)
        def _():
            head_copy(step + HEAD_BUFS - 1).start()

        head_copy(step).wait()
        where = pl.ds(pl.multiple_of(step * HEAD_TILE, HEAD_TILE), HEAD_TILE)
        return merge(total, head_tile(head_buf[lax.rem(step, HEAD_BUFS)], where))

    total = lax.fori_loop(0, head_full, head_step, empty)
    if head_rest:
        rest_copy.wait()
        where = pl.ds(head_full * HEAD_TILE, head_rest)
        total = merge(total, head_tile(head_buf[HEAD_BUFS, :head_rest, :], where))

    stat[0:1, :] = knn_max
    stat[1:2, :] = knn_sum
    stat[2:3, :] = total[0]
    stat[3:4, :] = total[1]
    stat[4:8, :] = over_ref[4:8, :]
    own = [
        pltpu.make_async_copy(send.at[0], recv_hbm.at[0], own_sem.at[0]),
        pltpu.make_async_copy(col_ref.at[me], rcol_hbm.at[0], own_sem.at[1]),
        pltpu.make_async_copy(logit, logit_hbm, own_sem.at[2]),
        pltpu.make_async_copy(stat, rstat_hbm.at[0], own_sem.at[3]),
    ]
    for copy in own:
        copy.start()
    for k in range(1, group):
        stat_copy(k).start()
    for copy in own + handed:
        copy.wait()
    for k in range(1, group):
        stat_copy(k).wait()
        cols_copy(k).wait()
        if k not in late:
            data_copy(k).wait()


def combine(stat, row):
    group = stat.shape[0]
    top = stat[0, row : row + 1, :]
    for k in range(1, group):
        top = jnp.maximum(top, stat[k, row : row + 1, :])
    acc = jnp.zeros((1, LANES), jnp.float32)
    for k in range(group):
        acc = acc + stat[k, row + 1 : row + 2, :] * jnp.exp(stat[k, row : row + 1, :] - top)
    return top, acc


def clear_hists(hists):
    def clear(i, carry):
        where = pl.ds(pl.multiple_of(i * CLEAR, CLEAR), CLEAR)
        for hist in hists:
            hist[where, :] = jnp.zeros((CLEAR, LANES), jnp.float32)
        return carry

    lax.fori_loop(0, hists[0].shape[0] // CLEAR, clear, 0)


def add_source(half, chunk, base, col_ref, hists, knn_max):
    chunk[...] = jnp.exp(chunk[...] - knn_max)

    def add_rows(j, count):
        for i in range(count):
            row = chunk[pl.ds(j + i, 1), :]
            low = hists[2 * (i % (HISTS // 2))]
            high = hists[2 * (i % (HISTS // 2)) + 1]
            a = col_ref[base + j + i]
            low[pl.ds(a, 1), :] = low[pl.ds(a, 1), :] + row
            b = col_ref[base + half + j + i]
            high[pl.ds(b, 1), :] = high[pl.ds(b, 1), :] + row

    def step(t, carry):
        add_rows(t * ROWS, ROWS)
        return carry

    lax.fori_loop(0, half // ROWS, step, 0)
    if half % ROWS:
        add_rows(half // ROWS * ROWS, half % ROWS)


def total_of(hists, where):
    low, high = hists[0][where, :], hists[1][where, :]
    for hist in range(2, HISTS, 2):
        low = low + hists[hist][where, :]
        high = high + hists[hist + 1][where, :]
    return low + pltpu.roll(high, LANES // 2, 1)


def first_kernel(group, half, slots, col_ref, stat, recv_hbm, part_ref, recv, *refs):
    hists, recv_sem = refs[:HISTS], refs[HISTS]
    late = late_chunks(group)
    first = [0] + list(range(late[len(late) // 2 - 1] + 1, late[len(late) // 2]))

    def fetch(k, i):
        return pltpu.make_async_copy(recv_hbm.at[k], recv.at[i], recv_sem.at[i])

    for i, k in enumerate(first):
        fetch(k, i).start()
    knn_max, unused = combine(stat, 0)
    clear_hists(hists)

    def one_source(i, carry):
        k = jnp.where(i == 0, 0, first[1] - 1 + i)
        fetch(k, i).wait()
        add_source(half, recv.at[i], k * slots, col_ref, hists, knn_max)
        return carry

    lax.fori_loop(0, len(first), one_source, 0)

    def fold(i, carry):
        where = pl.ds(pl.multiple_of(i * CLEAR, CLEAR), CLEAR)
        part_ref[where, :] = total_of(hists, where)
        return carry

    lax.fori_loop(0, part_ref.shape[0] // CLEAR, fold, 0)


def last_kernel(group, half, slots, col_ref, mix_ref, stat, logit_hbm, part_hbm, *refs):
    late = late_chunks(group)
    late_hbm, refs = refs[: len(late)], refs[len(late) :]
    out_ref, sum_ref, recv, logit, part = refs[:5]
    hists, (recv_sem, logit_sem) = refs[5 : 5 + HISTS], refs[5 + HISTS :]
    vocab = logit_hbm.shape[0]

    def fetch(i):
        return pltpu.make_async_copy(late_hbm[i], recv.at[i], recv_sem.at[i])

    for i in range(len(late)):
        fetch(i).start()
    whole = [
        pltpu.make_async_copy(logit_hbm, logit, logit_sem.at[0]),
        pltpu.make_async_copy(part_hbm, part, logit_sem.at[1]),
    ]
    for copy in whole:
        copy.start()

    knn_max, knn_sum = combine(stat, 0)
    lm_max, lm_sum = combine(stat, 2)
    over = stat[0, 4:5, :]
    for k in range(1, group):
        over = jnp.maximum(over, stat[k, 4:5, :])
    sum_ref[0:1, :] = knn_max
    sum_ref[1:2, :] = knn_sum
    sum_ref[2:3, :] = lm_max
    sum_ref[3:4, :] = lm_sum
    sum_ref[4:8, :] = jnp.broadcast_to(over, (4, LANES))

    clear_hists(hists)
    for i in range(len(late)):
        fetch(i).wait()

    def one_source(i, carry):
        k = jnp.where(i < len(late) // 2, i + 1, i + group - len(late))
        add_source(half, recv.at[i], k * slots, col_ref, hists, knn_max)
        return carry

    lax.fori_loop(0, len(late), one_source, 0)
    for copy in whole:
        copy.wait()

    mix = mix_ref[0]
    knn_scale = mix / knn_sum
    lm_scale = (1.0 - mix) / lm_sum

    def tile(start, count):
        where = pl.ds(start, count)
        hist = part[where, :] + total_of(hists, where)
        prob = hist * knn_scale + jnp.exp(logit[where, :] - lm_max) * lm_scale
        return jnp.log(prob)

    full = vocab // LANES

    def write(i, carry):
        start = pl.multiple_of(i * LANES, LANES)
        out_ref[:, pl.ds(start, LANES)] = tile(start, LANES).T[: LANES // 2, :]
        return carry

    lax.fori_loop(0, full, write, 0)
    rest = vocab - full * LANES
    if rest:
        last = jnp.concatenate(
            [tile(full * LANES, rest), jnp.zeros((LANES - rest, LANES), jnp.float32)], axis=0
        )
        out_ref[:, full * LANES :] = last.T[: LANES // 2, :rest]


def solution(mesh):
    group = mesh.shape["model"]

    def local_step(queries, w_shard, key_shard, tok_shard, temperature, mix_weight):
        row_count, depth = queries.shape
        vocab, n_local = w_shard.shape[1], key_shard.shape[0]
        mean = n_local / group
        cap = round_up(int(mean + 4.5 * math.sqrt(mean)), 16)
        half = cap // 2
        slot_rows = round_up(cap, LANES) // LANES
        slots = slot_rows * LANES

        order_tok, order_idx = lax.sort(
            (tok_shard, lax.iota(jnp.int32, n_local)), num_keys=1, is_stable=False
        )
        pad = (slot_rows + 8) * LANES
        fill = jnp.zeros((pad,), jnp.int32)
        shape_2d = ((n_local + pad) // LANES, LANES)
        tok_2d = jnp.concatenate([order_tok, fill]).reshape(shape_2d)
        idx_2d = jnp.concatenate([order_idx, fill]).reshape(shape_2d)

        smem = pl.BlockSpec(memory_space=pltpu.SMEM)
        vmem = pl.BlockSpec(memory_space=pltpu.VMEM)
        hbm = pl.BlockSpec(memory_space=pl.ANY)
        table = jax.ShapeDtypeStruct((group, slot_rows, LANES), jnp.int32)
        cols, idx, over = pl.pallas_call(
            functools.partial(slot_kernel, group, vocab, cap, slot_rows, n_local),
            out_shape=(
                table,
                jax.ShapeDtypeStruct((group * slot_rows, LANES), jnp.int32),
                jax.ShapeDtypeStruct((8, LANES), jnp.float32),
            ),
            in_specs=[vmem, vmem],
            out_specs=(vmem, vmem, vmem),
            name="slots",
        )(tok_2d, idx_2d)

        dma = pltpu.SemaphoreType.DMA
        logit = pltpu.VMEM((vocab, LANES), jnp.float32)
        late = late_chunks(group)
        chunk = jax.ShapeDtypeStruct((half, LANES), jnp.float32)
        recv, rcols, rstat, logits, *handed = pl.pallas_call(
            functools.partial(exchange_kernel, group, half, slot_rows),
            out_shape=(
                jax.ShapeDtypeStruct((group, half, LANES), jnp.float32),
                table,
                jax.ShapeDtypeStruct((group, 8, LANES), jnp.float32),
                jax.ShapeDtypeStruct((vocab, LANES), jnp.float32),
                *[chunk] * len(late),
            ),
            in_specs=[smem, smem, vmem, vmem, vmem, hbm, hbm],
            out_specs=(hbm,) * (4 + len(late)),
            scratch_shapes=[
                pltpu.VMEM((KEY_BUFS, KEY_TILE, depth), jnp.bfloat16),
                pltpu.VMEM((HEAD_BUFS + 1, HEAD_TILE, depth), jnp.bfloat16),
                pltpu.VMEM((depth, LANES), jnp.bfloat16),
                pltpu.VMEM((n_local, LANES), jnp.float32),
                pltpu.VMEM((group, half, LANES), jnp.float32),
                pltpu.VMEM((8, LANES), jnp.float32),
                logit,
                dma((KEY_BUFS,)), dma((HEAD_BUFS + 1,)), dma((group,)), dma((group,)),
                dma((group,)), dma((group,)), dma((group,)), dma((group,)), dma((4,)), dma((len(late),)),
            ],
            compiler_params=pltpu.CompilerParams(
                collective_id=0, has_side_effects=True, vmem_limit_bytes=VMEM_LIMIT
            ),
            name="exchange",
        )(idx.reshape(-1), temperature, queries, over, cols, key_shard, w_shard.T)

        landed = [
            lax.ppermute(handed[i], "model", [(d, (d + k) % group) for d in range(group)])
            for i, k in enumerate(late)
        ]
        flat_cols = rcols.reshape(-1)
        hist_rows = round_up(vocab + 1, CLEAR)
        hists = [pltpu.VMEM((hist_rows, LANES), jnp.float32)] * HISTS
        early = group - len(late)
        part = pl.pallas_call(
            functools.partial(first_kernel, group, half, slots),
            out_shape=jax.ShapeDtypeStruct((hist_rows, LANES), jnp.float32),
            in_specs=[smem, vmem, hbm],
            out_specs=vmem,
            scratch_shapes=[pltpu.VMEM((early, half, LANES), jnp.float32), *hists, dma((early,))],
            compiler_params=pltpu.CompilerParams(vmem_limit_bytes=VMEM_LIMIT),
            cost_estimate=pl.CostEstimate(flops=10**9, bytes_accessed=10**7, transcendentals=0),
            name="first",
        )(flat_cols, rstat, recv)
        fast, sums = pl.pallas_call(
            functools.partial(last_kernel, group, half, slots),
            out_shape=(
                jax.ShapeDtypeStruct((row_count, vocab), jnp.float32),
                jax.ShapeDtypeStruct((8, LANES), jnp.float32),
            ),
            in_specs=[smem, smem, vmem, hbm, hbm] + [hbm] * len(late),
            out_specs=(vmem, vmem),
            scratch_shapes=[
                pltpu.VMEM((len(late), half, LANES), jnp.float32),
                logit,
                hists[0],
                *hists,
                dma((len(late),)), dma((2,)),
            ],
            compiler_params=pltpu.CompilerParams(vmem_limit_bytes=VMEM_LIMIT),
            name="last",
        )(flat_cols, mix_weight, rstat, logits, part, *landed)

        def dense(unused):
            me = lax.axis_index("model")
            row_max, row_total = sums[0, :row_count], sums[1, :row_count]
            lm_max, lm_total = sums[2, :row_count], sums[3, :row_count]
            cross_dot = jnp.einsum("bd,nd->nb", queries, key_shard, preferred_element_type=jnp.float32)
            key_sq = jnp.sum(jnp.square(key_shard.astype(jnp.float32)), axis=1)
            scores = (2.0 * cross_dot - key_sq[:, None]) / temperature[0]
            weights = jnp.exp(scores - row_max[None, :])
            ring = [(i, (i + 1) % group) for i in range(group)]

            def turn(k, acc):
                acc = lax.ppermute(acc, "model", ring)
                col = tok_shard - lax.rem(me + group - 1 - k, group) * vocab
                col = jnp.where((col >= 0) & (col < vocab), col, vocab)
                return acc.at[col].add(weights)

            acc = jnp.zeros((vocab + 1, row_count), jnp.float32)
            acc = lax.fori_loop(0, group, turn, acc)
            logit = jnp.dot(queries, w_shard, preferred_element_type=jnp.float32)
            p_lm = jnp.exp(logit - lm_max[:, None]) / lm_total[:, None]
            p_knn = acc[:vocab].T / row_total[:, None]
            mix_value = mix_weight[0]
            return jnp.log(mix_value * p_knn + (1.0 - mix_value) * p_lm)

        return lax.cond(sums[4, 0] > 0.0, dense, lambda kept: kept, fast)

    return jax.shard_map(
        local_step,
        mesh=mesh,
        in_specs=(P("data", None), P(None, "model"), P("model", None), P("model"), P(), P()),
        out_specs=P("data", "model"),
        check_vma=False,
    )
```

```python
import functools
import math

import jax
import jax.numpy as jnp
from jax import lax
from jax.experimental import pallas as pl
from jax.experimental.pallas import tpu as pltpu
from jax.sharding import PartitionSpec as P

MESH = pl.DeviceIdType.MESH
LANES = 128
KEY_TILE = 512
KEY_BUFS = 4
HEAD_TILE = 512
HEAD_BUFS = 3
HISTS = 8
ROWS = 16
CLEAR = 216
VMEM_LIMIT = 60 * 1024 * 1024


def round_up(value, step):
    return (value + step - 1) // step * step


def slot_kernel(group, vocab, cap, rows, n_local, tok_ref, ord_ref, col_ref, idx_ref, over_ref):
    lane = lax.broadcasted_iota(jnp.int32, (rows, LANES), 1)
    slot = lax.broadcasted_iota(jnp.int32, (rows, LANES), 0) * LANES + lane
    tokens = tok_ref[: n_local // LANES, :]

    def below(limit):
        return jnp.sum((tokens < limit).astype(jnp.int32))

    starts = [0] + [below(d * vocab) for d in range(1, group)] + [n_local]
    most = jnp.int32(0)
    for d in range(group):
        start, count = starts[d], starts[d + 1] - starts[d]
        most = jnp.maximum(most, count)
        row, off = start // LANES, start % LANES
        shift = (LANES - off) % LANES

        def shifted(ref):
            low = pltpu.roll(ref[pl.ds(row, rows), :], shift, 1)
            high = pltpu.roll(ref[pl.ds(row + 1, rows), :], shift, 1)
            return jnp.where(lane < LANES - off, low, high)

        used = slot < count
        col_ref[d] = jnp.where(used, shifted(tok_ref) - d * vocab, vocab)
        idx_ref[d * rows : (d + 1) * rows, :] = jnp.where(used, shifted(ord_ref), 0)
    over = jnp.where(most > cap, 1.0, 0.0)
    over_ref[...] = jnp.full((8, LANES), over, jnp.float32)


def late_chunks(group):
    near = min(3, group // 2 - 1)
    return [k for k in range(1, group) if k <= near or k >= group - near]


def exchange_kernel(
    group, half, rows, idx_hbm, temp_ref, query_ref, over_ref, col_ref, key_hbm, head_hbm,
    recv_hbm, rcol_hbm, rstat_hbm, logit_hbm, *refs,
):
    late = late_chunks(group)
    late_hbm, refs = refs[: len(late)], refs[len(late) :]
    (
        key_buf, head_buf, turned, score, send, stat, logit,
        key_sem, head_sem, data_send, data_recv, col_send, col_recv,
        stat_send, stat_recv, own_sem, late_sem, idx_ref, idx_sem,
    ) = refs
    idx_copy = pltpu.make_async_copy(idx_hbm, idx_ref, idx_sem)
    idx_copy.start()
    me = lax.axis_index("model")
    n_local, vocab = key_hbm.shape[0], head_hbm.shape[0]
    slots = rows * LANES
    mid = group // 2

    def peer(k):
        return {"model": lax.rem(me + k, group)}

    barrier = pltpu.get_barrier_semaphore()
    for k in range(1, group):
        pl.semaphore_signal(barrier, inc=1, device_id=peer(k), device_id_type=MESH)

    def key_copy(step):
        return pltpu.make_async_copy(
            key_hbm.at[pl.ds(step * KEY_TILE, KEY_TILE), :],
            key_buf.at[lax.rem(step, KEY_BUFS)],
            key_sem.at[lax.rem(step, KEY_BUFS)],
        )

    head_full = vocab // HEAD_TILE
    head_rest = vocab - head_full * HEAD_TILE

    def head_copy(step):
        return pltpu.make_async_copy(
            head_hbm.at[pl.ds(step * HEAD_TILE, HEAD_TILE), :],
            head_buf.at[lax.rem(step, HEAD_BUFS)],
            head_sem.at[lax.rem(step, HEAD_BUFS)],
        )

    key_steps = n_local // KEY_TILE
    for step in range(KEY_BUFS - 1):
        key_copy(step).start()

    temp = temp_ref[0]
    query = query_ref[...].astype(jnp.float32)
    turned[...] = jnp.concatenate([query, query], axis=0).T.astype(jnp.bfloat16)

    def merge(total, tile):
        top, acc = total
        new = jnp.maximum(top, jnp.max(tile, axis=0, keepdims=True))
        acc = acc * jnp.exp(top - new) + jnp.sum(jnp.exp(tile - new), axis=0, keepdims=True)
        return new, acc

    empty = (jnp.full((1, LANES), -3e38, jnp.float32), jnp.zeros((1, LANES), jnp.float32))

    def score_step(step, total):
        @pl.when(step + KEY_BUFS - 1 < key_steps)
        def _():
            key_copy(step + KEY_BUFS - 1).start()

        key_copy(step).wait()
        keys = key_buf[lax.rem(step, KEY_BUFS)]
        cross = jnp.dot(keys, turned[...], preferred_element_type=jnp.float32)
        wide = keys.astype(jnp.float32)
        square = jnp.sum(wide * wide, axis=1, keepdims=True)
        tile = (2.0 * cross - square) / temp
        score[pl.ds(pl.multiple_of(step * KEY_TILE, KEY_TILE), KEY_TILE), :] = tile
        return merge(total, tile)

    knn_max, knn_sum = lax.fori_loop(0, key_steps, score_step, empty)

    for step in range(HEAD_BUFS - 1):
        head_copy(step).start()

    pl.semaphore_wait(barrier, group - 1)
    idx_copy.wait()

    left = lax.broadcasted_iota(jnp.int32, (1, LANES), 1) < LANES // 2

    def remote(src, dst, send_sem, recv_sem, k):
        return pltpu.make_async_remote_copy(
            src_ref=src, dst_ref=dst, send_sem=send_sem, recv_sem=recv_sem,
            device_id=peer(k), device_id_type=MESH,
        )

    def data_copy(k):
        return remote(send.at[k], recv_hbm.at[k], data_send.at[k], data_recv.at[k], k)

    def cols_copy(k):
        return remote(col_ref.at[lax.rem(me + k, group)], rcol_hbm.at[k], col_send.at[k], col_recv.at[k], k)

    def stat_copy(k):
        return remote(stat, rstat_hbm.at[k], stat_send.at[k], stat_recv.at[k], k)

    def pack(k):
        base = lax.rem(me + k, group) * slots

        def tile(t, carry):
            for i in range(8):
                j = t * 8 + i
                a = idx_ref[base + j]
                b = idx_ref[base + half + j]
                row = jnp.where(left, score[pl.ds(a, 1), :], score[pl.ds(b, 1), :])
                send[k, pl.ds(j, 1), :] = row
            return carry

        lax.fori_loop(0, half // 8, tile, 0, unroll=2)

    for k in range(1, group):
        cols_copy(k).start()
    order = [mid]
    for k in range(1, mid):
        order += [mid - k, mid + k]
    waiting, handed = None, []
    for k in order:
        pack(k)
        if waiting is not None:
            waiting.start()
        if k in late:
            waiting = pltpu.make_async_copy(send.at[k], late_hbm[late.index(k)], late_sem.at[late.index(k)])
            handed.append(waiting)
        else:
            waiting = data_copy(k)
    pack(0)
    waiting.start()

    def head_tile(tile, where):
        tile = jnp.dot(tile, turned[...], preferred_element_type=jnp.float32)
        logit[where, :] = tile
        return tile

    rest_copy = pltpu.make_async_copy(
        head_hbm.at[pl.ds(head_full * HEAD_TILE, head_rest), :],
        head_buf.at[HEAD_BUFS, pl.ds(0, head_rest), :],
        head_sem.at[HEAD_BUFS],
    )
    if head_rest:
        rest_copy.start()

    def head_step(step, total):
        @pl.when(step + HEAD_BUFS - 1 < head_full)
        def _():
            head_copy(step + HEAD_BUFS - 1).start()

        head_copy(step).wait()
        where = pl.ds(pl.multiple_of(step * HEAD_TILE, HEAD_TILE), HEAD_TILE)
        return merge(total, head_tile(head_buf[lax.rem(step, HEAD_BUFS)], where))

    total = lax.fori_loop(0, head_full, head_step, empty)
    if head_rest:
        rest_copy.wait()
        where = pl.ds(head_full * HEAD_TILE, head_rest)
        total = merge(total, head_tile(head_buf[HEAD_BUFS, :head_rest, :], where))

    stat[0:1, :] = knn_max
    stat[1:2, :] = knn_sum
    stat[2:3, :] = total[0]
    stat[3:4, :] = total[1]
    stat[4:8, :] = over_ref[4:8, :]
    own = [
        pltpu.make_async_copy(send.at[0], recv_hbm.at[0], own_sem.at[0]),
        pltpu.make_async_copy(col_ref.at[me], rcol_hbm.at[0], own_sem.at[1]),
        pltpu.make_async_copy(logit, logit_hbm, own_sem.at[2]),
        pltpu.make_async_copy(stat, rstat_hbm.at[0], own_sem.at[3]),
    ]
    for copy in own:
        copy.start()
    for k in range(1, group):
        stat_copy(k).start()
    for copy in own + handed:
        copy.wait()
    for k in range(1, group):
        stat_copy(k).wait()
        cols_copy(k).wait()
        if k not in late:
            data_copy(k).wait()


def combine(stat, row):
    group = stat.shape[0]
    top = stat[0, row : row + 1, :]
    for k in range(1, group):
        top = jnp.maximum(top, stat[k, row : row + 1, :])
    acc = jnp.zeros((1, LANES), jnp.float32)
    for k in range(group):
        acc = acc + stat[k, row + 1 : row + 2, :] * jnp.exp(stat[k, row : row + 1, :] - top)
    return top, acc


def clear_hists(hists):
    def clear(i, carry):
        where = pl.ds(pl.multiple_of(i * CLEAR, CLEAR), CLEAR)
        for hist in hists:
            hist[where, :] = jnp.zeros((CLEAR, LANES), jnp.float32)
        return carry

    lax.fori_loop(0, hists[0].shape[0] // CLEAR, clear, 0)


def add_source(half, chunk, base, col_ref, hists, knn_max):
    chunk[...] = jnp.exp(chunk[...] - knn_max)

    def add_rows(j, count):
        for i in range(count):
            row = chunk[pl.ds(j + i, 1), :]
            low = hists[2 * (i % (HISTS // 2))]
            high = hists[2 * (i % (HISTS // 2)) + 1]
            a = col_ref[base + j + i]
            low[pl.ds(a, 1), :] = low[pl.ds(a, 1), :] + row
            b = col_ref[base + half + j + i]
            high[pl.ds(b, 1), :] = high[pl.ds(b, 1), :] + row

    def step(t, carry):
        add_rows(t * ROWS, ROWS)
        return carry

    lax.fori_loop(0, half // ROWS, step, 0)
    if half % ROWS:
        add_rows(half // ROWS * ROWS, half % ROWS)


def total_of(hists, where):
    low, high = hists[0][where, :], hists[1][where, :]
    for hist in range(2, HISTS, 2):
        low = low + hists[hist][where, :]
        high = high + hists[hist + 1][where, :]
    return low + pltpu.roll(high, LANES // 2, 1)


def first_kernel(group, half, slots, col_hbm, stat, recv_hbm, part_ref, recv, *refs):
    hists, (recv_sem, col_ref, col_sem) = refs[:HISTS], refs[HISTS:]
    col_copy = pltpu.make_async_copy(col_hbm, col_ref, col_sem)
    col_copy.start()
    late = late_chunks(group)
    first = [0] + list(range(late[len(late) // 2 - 1] + 1, late[len(late) // 2]))

    def fetch(k, i):
        return pltpu.make_async_copy(recv_hbm.at[k], recv.at[i], recv_sem.at[i])

    for i, k in enumerate(first):
        fetch(k, i).start()
    knn_max, unused = combine(stat, 0)
    clear_hists(hists)
    col_copy.wait()

    def one_source(i, carry):
        k = jnp.where(i == 0, 0, first[1] - 1 + i)
        fetch(k, i).wait()
        add_source(half, recv.at[i], k * slots, col_ref, hists, knn_max)
        return carry

    lax.fori_loop(0, len(first), one_source, 0)

    def fold(i, carry):
        where = pl.ds(pl.multiple_of(i * CLEAR, CLEAR), CLEAR)
        part_ref[where, :] = total_of(hists, where)
        return carry

    lax.fori_loop(0, part_ref.shape[0] // CLEAR, fold, 0)


def last_kernel(group, half, slots, col_hbm, mix_ref, stat, logit_hbm, part_hbm, *refs):
    late = late_chunks(group)
    late_hbm, refs = refs[: len(late)], refs[len(late) :]
    out_ref, sum_ref, recv, logit, part = refs[:5]
    hists, (recv_sem, logit_sem, col_ref, col_sem) = refs[5 : 5 + HISTS], refs[5 + HISTS :]
    col_copy = pltpu.make_async_copy(col_hbm, col_ref, col_sem)
    col_copy.start()
    vocab = logit_hbm.shape[0]

    def fetch(i):
        return pltpu.make_async_copy(late_hbm[i], recv.at[i], recv_sem.at[i])

    for i in range(len(late)):
        fetch(i).start()
    whole = [
        pltpu.make_async_copy(logit_hbm, logit, logit_sem.at[0]),
        pltpu.make_async_copy(part_hbm, part, logit_sem.at[1]),
    ]
    for copy in whole:
        copy.start()

    knn_max, knn_sum = combine(stat, 0)
    lm_max, lm_sum = combine(stat, 2)
    over = stat[0, 4:5, :]
    for k in range(1, group):
        over = jnp.maximum(over, stat[k, 4:5, :])
    sum_ref[0:1, :] = knn_max
    sum_ref[1:2, :] = knn_sum
    sum_ref[2:3, :] = lm_max
    sum_ref[3:4, :] = lm_sum
    sum_ref[4:8, :] = jnp.broadcast_to(over, (4, LANES))

    clear_hists(hists)
    col_copy.wait()
    for i in range(len(late)):
        fetch(i).wait()

    def one_source(i, carry):
        k = jnp.where(i < len(late) // 2, i + 1, i + group - len(late))
        add_source(half, recv.at[i], k * slots, col_ref, hists, knn_max)
        return carry

    lax.fori_loop(0, len(late), one_source, 0)
    for copy in whole:
        copy.wait()

    mix = mix_ref[0]
    knn_scale = mix / knn_sum
    lm_scale = (1.0 - mix) / lm_sum

    def tile(start, count):
        where = pl.ds(start, count)
        hist = part[where, :] + total_of(hists, where)
        prob = hist * knn_scale + jnp.exp(logit[where, :] - lm_max) * lm_scale
        return jnp.log(prob)

    full = vocab // LANES

    def write(i, carry):
        start = pl.multiple_of(i * LANES, LANES)
        out_ref[:, pl.ds(start, LANES)] = tile(start, LANES).T[: LANES // 2, :]
        return carry

    lax.fori_loop(0, full, write, 0)
    rest = vocab - full * LANES
    if rest:
        last = jnp.concatenate(
            [tile(full * LANES, rest), jnp.zeros((LANES - rest, LANES), jnp.float32)], axis=0
        )
        out_ref[:, full * LANES :] = last.T[: LANES // 2, :rest]


def solution(mesh):
    group = mesh.shape["model"]

    def local_step(queries, w_shard, key_shard, tok_shard, temperature, mix_weight):
        row_count, depth = queries.shape
        vocab, n_local = w_shard.shape[1], key_shard.shape[0]
        mean = n_local / group
        cap = round_up(int(mean + 4.5 * math.sqrt(mean)), 16)
        half = cap // 2
        slot_rows = round_up(cap, LANES) // LANES
        slots = slot_rows * LANES

        order_tok, order_idx = lax.sort(
            (tok_shard, lax.iota(jnp.int32, n_local)), num_keys=1, is_stable=False
        )
        pad = (slot_rows + 8) * LANES
        fill = jnp.zeros((pad,), jnp.int32)
        shape_2d = ((n_local + pad) // LANES, LANES)
        tok_2d = jnp.concatenate([order_tok, fill]).reshape(shape_2d)
        idx_2d = jnp.concatenate([order_idx, fill]).reshape(shape_2d)

        smem = pl.BlockSpec(memory_space=pltpu.SMEM)
        vmem = pl.BlockSpec(memory_space=pltpu.VMEM)
        hbm = pl.BlockSpec(memory_space=pl.ANY)
        table = jax.ShapeDtypeStruct((group, slot_rows, LANES), jnp.int32)
        cols, idx, over = pl.pallas_call(
            functools.partial(slot_kernel, group, vocab, cap, slot_rows, n_local),
            out_shape=(
                table,
                jax.ShapeDtypeStruct((group * slot_rows, LANES), jnp.int32),
                jax.ShapeDtypeStruct((8, LANES), jnp.float32),
            ),
            in_specs=[vmem, vmem],
            out_specs=(vmem, vmem, vmem),
            name="slots",
        )(tok_2d, idx_2d)

        dma = pltpu.SemaphoreType.DMA
        index = pltpu.SMEM((group * slots,), jnp.int32)
        logit = pltpu.VMEM((vocab, LANES), jnp.float32)
        late = late_chunks(group)
        chunk = jax.ShapeDtypeStruct((half, LANES), jnp.float32)
        recv, rcols, rstat, logits, *handed = pl.pallas_call(
            functools.partial(exchange_kernel, group, half, slot_rows),
            out_shape=(
                jax.ShapeDtypeStruct((group, half, LANES), jnp.float32),
                table,
                jax.ShapeDtypeStruct((group, 8, LANES), jnp.float32),
                jax.ShapeDtypeStruct((vocab, LANES), jnp.float32),
                *[chunk] * len(late),
            ),
            in_specs=[hbm, smem, vmem, vmem, vmem, hbm, hbm],
            out_specs=(hbm,) * (4 + len(late)),
            scratch_shapes=[
                pltpu.VMEM((KEY_BUFS, KEY_TILE, depth), jnp.bfloat16),
                pltpu.VMEM((HEAD_BUFS + 1, HEAD_TILE, depth), jnp.bfloat16),
                pltpu.VMEM((depth, LANES), jnp.bfloat16),
                pltpu.VMEM((n_local, LANES), jnp.float32),
                pltpu.VMEM((group, half, LANES), jnp.float32),
                pltpu.VMEM((8, LANES), jnp.float32),
                logit,
                dma((KEY_BUFS,)), dma((HEAD_BUFS + 1,)), dma((group,)), dma((group,)),
                dma((group,)), dma((group,)), dma((group,)), dma((group,)), dma((4,)), dma((len(late),)),
                index, dma,
            ],
            compiler_params=pltpu.CompilerParams(
                collective_id=0, has_side_effects=True, vmem_limit_bytes=VMEM_LIMIT
            ),
            name="exchange",
        )(idx.reshape(-1), temperature, queries, over, cols, key_shard, w_shard.T)

        landed = [
            lax.ppermute(handed[i], "model", [(d, (d + k) % group) for d in range(group)])
            for i, k in enumerate(late)
        ]
        flat_cols = rcols.reshape(-1)
        hist_rows = round_up(vocab + 1, CLEAR)
        hists = [pltpu.VMEM((hist_rows, LANES), jnp.float32)] * HISTS
        early = group - len(late)
        part = pl.pallas_call(
            functools.partial(first_kernel, group, half, slots),
            out_shape=jax.ShapeDtypeStruct((hist_rows, LANES), jnp.float32),
            in_specs=[hbm, vmem, hbm],
            out_specs=vmem,
            scratch_shapes=[pltpu.VMEM((early, half, LANES), jnp.float32), *hists, dma((early,)), index, dma],
            compiler_params=pltpu.CompilerParams(vmem_limit_bytes=VMEM_LIMIT),
            cost_estimate=pl.CostEstimate(flops=10**9, bytes_accessed=10**7, transcendentals=0),
            name="first",
        )(flat_cols, rstat, recv)
        fast, sums = pl.pallas_call(
            functools.partial(last_kernel, group, half, slots),
            out_shape=(
                jax.ShapeDtypeStruct((row_count, vocab), jnp.float32),
                jax.ShapeDtypeStruct((8, LANES), jnp.float32),
            ),
            in_specs=[hbm, smem, vmem, hbm, hbm] + [hbm] * len(late),
            out_specs=(vmem, vmem),
            scratch_shapes=[
                pltpu.VMEM((len(late), half, LANES), jnp.float32),
                logit,
                hists[0],
                *hists,
                dma((len(late),)), dma((2,)), index, dma,
            ],
            compiler_params=pltpu.CompilerParams(vmem_limit_bytes=VMEM_LIMIT),
            name="last",
        )(flat_cols, mix_weight, rstat, logits, part, *landed)

        def dense(unused):
            me = lax.axis_index("model")
            row_max, row_total = sums[0, :row_count], sums[1, :row_count]
            lm_max, lm_total = sums[2, :row_count], sums[3, :row_count]
            cross_dot = jnp.einsum("bd,nd->nb", queries, key_shard, preferred_element_type=jnp.float32)
            key_sq = jnp.sum(jnp.square(key_shard.astype(jnp.float32)), axis=1)
            scores = (2.0 * cross_dot - key_sq[:, None]) / temperature[0]
            weights = jnp.exp(scores - row_max[None, :])
            ring = [(i, (i + 1) % group) for i in range(group)]

            def turn(k, acc):
                acc = lax.ppermute(acc, "model", ring)
                col = tok_shard - lax.rem(me + group - 1 - k, group) * vocab
                col = jnp.where((col >= 0) & (col < vocab), col, vocab)
                return acc.at[col].add(weights)

            acc = jnp.zeros((vocab + 1, row_count), jnp.float32)
            acc = lax.fori_loop(0, group, turn, acc)
            logit = jnp.dot(queries, w_shard, preferred_element_type=jnp.float32)
            p_lm = jnp.exp(logit - lm_max[:, None]) / lm_total[:, None]
            p_knn = acc[:vocab].T / row_total[:, None]
            mix_value = mix_weight[0]
            return jnp.log(mix_value * p_knn + (1.0 - mix_value) * p_lm)

        return lax.cond(sums[4, 0] > 0.0, dense, lambda kept: kept, fast)

    return jax.shard_map(
        local_step,
        mesh=mesh,
        in_specs=(P("data", None), P(None, "model"), P("model", None), P("model"), P(), P()),
        out_specs=P("data", "model"),
        check_vma=False,
    )
```
